32 devices in a mesh: section: 4 (over y, x), vocab: 8 (over z, core).
Axes of the slice: x: 2, y: 2, z: 4, core: 2. Of those that a mesh axis runs over, the one named last changes fastest.
Arguments:
- hidden: bfloat16 [512, 4608], P('section', 'vocab'), may hold values from -6 to 6
- slab: bfloat16 [16384, 4608], P('vocab', 'section'), may hold values from -0.29882812 to 0.29882812
- token_ids: int32 [512], P('section'), may hold values from 0 to 16383
- target_ids: int32 [512], P('section'), may hold values from 0 to 16383
- input_cot: bfloat16 [512, 4608], P('section', 'vocab'), may hold values from -0.3984375 to 0.3984375
- loss_grad: float32 [512], P('section'), may hold values from 2 to 32
Outputs:
- token_loss: float32 [512], P('section')
- hidden_grad: bfloat16 [512, 4608], P('section', 'vocab')
- tied_grad: bfloat16 [16384, 4608], P('vocab', 'section')
The draws below stay inside these ranges and needn't reach their ends.
All inputs are finite; a program needn't handle non-finite values.
Results may differ from the reference program's by a relative error of at most 0.0047.
Values may be sent and summed in bfloat16 or wider, within the bound.
A program may use at most 64 MiB of HBM per device.

```python
import math
import jax
import jax.numpy as jnp
import numpy as np
from jax import lax

D = 4608
TOKENS = 512
VOCAB = 16384


def touch_ends(result, own_key, smallest, largest):
    place = [jax.random.randint(jax.random.fold_in(own_key, axis), (), 0, length) for axis, length in enumerate(result.shape)]
    widest = result.shape.index(max(result.shape))
    neighbour = place[:widest] + [(place[widest] + 1) % result.shape[widest]] + place[widest + 1:]
    return result.at[tuple(place)].set(smallest).at[tuple(neighbour)].set(largest)


def shard_levels(stream_key, shape, split, smallest, high):
    level = 1.0
    for position, shards_of in split:
        heights = jax.random.uniform(jax.random.fold_in(jax.random.fold_in(stream_key, 6), position), (shards_of,), jnp.float32, smallest / len(split), high / len(split))
        level = level * jnp.repeat(jnp.exp(heights), shape[position] // shards_of).reshape((-1,) + (1,) * (len(shape) - 1 - position))
    return level


def cumulative_ranks(amount, skew):
    weights = [(1 << 20) // math.isqrt(rank ** skew) + 1 for rank in range(1, amount + 1)]
    deviation = 1 + sum(weights) // (1 << 30)
    return np.cumsum(np.array([max(1, weight // deviation) for weight in weights]))


def ranked(rng, dims, count, skew):
    table = cumulative_ranks(count, skew)
    ticket = jax.random.randint(jax.random.fold_in(rng, 1), dims, 0, int(table[count - 1]))
    rank = jnp.searchsorted(jnp.asarray(table, jnp.int32), ticket, side="right")
    return jax.random.permutation(jax.random.fold_in(rng, 2), count)[rank].astype(jnp.int32)


def noise(own_key, extent, scale, reach, cuts=(), kind=jnp.bfloat16):
    result = scale * jax.random.normal(own_key, extent, jnp.float32)
    if cuts:
        result = result * shard_levels(own_key, extent, cuts, -0.22, 0.18)
    return jnp.clip(result, -reach, reach).astype(kind)


def setup_inputs(seed: int = 0) -> dict:
    key_of = jax.random.split(jax.random.key(seed), 7)
    return {
        "hidden": noise(key_of[0], (TOKENS, D), 1.0, 6.0, ((0, 4), (1, 8))),
        "slab": noise(key_of[1], (VOCAB, D), 0.05, 0.29882812, ((0, 8), (1, 4))),
        "token_ids": touch_ends(ranked(key_of[2], (TOKENS,), VOCAB, 2), jax.random.fold_in(key_of[2], 3), 0, VOCAB - 1).astype(jnp.int32),
        "target_ids": touch_ends(ranked(key_of[3], (TOKENS,), VOCAB, 2), jax.random.fold_in(key_of[3], 3), 0, VOCAB - 1).astype(jnp.int32),
        "input_cot": noise(key_of[4], (TOKENS, D), 0.05, 0.3984375, ((0, 4), (1, 8))),
        "loss_grad": jnp.clip(jnp.exp(math.log(32.0) - 2.7725887 * jax.random.uniform(key_of[5], (TOKENS,), jnp.float32) ** shard_levels(key_of[5], (TOKENS,), ((0, 4),), -0.2, 0.2)), 2.0, 32.0),
    }


logit_cap = 30.0

def reference(hidden, slab, token_ids, target_ids, input_cot, loss_grad):
    raw_logits = jnp.dot(hidden, slab.T, preferred_element_type=jnp.float32)
    capped = logit_cap * jnp.tanh(raw_logits / logit_cap)
    exp_logits = jnp.exp(capped)
    exp_total = lax.optimization_barrier(jnp.sum(exp_logits, axis=1))
    columns = jnp.arange(VOCAB, dtype=jnp.int32)
    target_hit = (target_ids[:, None] == columns[None, :]).astype(jnp.float32)
    picked = lax.optimization_barrier(jnp.sum(target_hit * capped, axis=1))
    token_loss = jnp.log(exp_total) - picked
    slope = 1.0 - (capped / logit_cap) ** 2
    dlogit = (loss_grad[:, None] * (exp_logits / exp_total[:, None] - target_hit) * slope).astype(jnp.bfloat16)
    hidden_grad = jnp.dot(dlogit, slab, preferred_element_type=jnp.float32).astype(jnp.bfloat16)
    head_grad = jnp.dot(dlogit.T, hidden, preferred_element_type=jnp.float32)
    onehot = (token_ids[:, None] == columns[None, :]).astype(jnp.bfloat16)
    embed_grad = jnp.dot(onehot.T, input_cot, preferred_element_type=jnp.float32) * math.sqrt(D)
    return (token_loss, hidden_grad, (head_grad + embed_grad).astype(jnp.bfloat16))
```

```python
import functools
import math

import jax
import jax.numpy as jnp
from jax import lax
from jax.experimental import pallas as pl
from jax.experimental.pallas import tpu as pltpu
from jax.sharding import PartitionSpec as P

logit_cap = 30.0
code_knee = 16.0
code_top = 32767.0
f32 = jnp.float32
bf16 = jnp.bfloat16


def encode(x):
    y = x / (jnp.abs(x) + code_knee) * code_top
    return jnp.floor(y + 0.5).astype(jnp.int32).astype(jnp.int16)


def decode(code):
    y = code.astype(jnp.int32).astype(f32) * (1.0 / code_top)
    return code_knee * y / (1.0 - jnp.abs(y))


def over_tokens(left, right):
    return lax.dot_general(
        left, right, (((1,), (1,)), ((), ())), preferred_element_type=jnp.float32
    )


def fused_kernel(
    dims, hid_hbm, cot_hbm, slab_hbm, tok_hbm, tgt_hbm, scale_hbm, loss, hgrad, tied,
    hid, cot, tok, tgt, scale,
    slab, zg, hq, hm, h, snd, rcv, own, cq, cm, cf, ids, tid_tx, cap, ex, stat_tx, stat_rx,
    dl, gt, px_rx, gs, zr, fin,
    in_sem, zr_s, zr_r, zl_s, zl_r, pl_s, pl_r, mt_s, mt_r, cp_s, cp_r, cr_s, cl_s, cz_r,
    cm_s, cm_r, id_s, id_r, rs_s, rs_r, st_s, st_r, ag_s, ag_r, px_s, px_r, g_s, g_r, f_s, f_r,
):
    S, V = dims
    Z = V // 2
    W, T = hid.shape
    R, Q = slab.shape
    half = R // 2
    s = lax.axis_index("section")
    v = lax.axis_index("vocab")
    z = v // 2
    c = v % 2
    mate = z * 2 + 1 - c
    nx, ny, far = s ^ 1, s ^ 2, s ^ 3
    tile = 256

    def rc(src, dst, ssem, rsem, dev):
        return pltpu.make_async_remote_copy(
            src_ref=src, dst_ref=dst, send_sem=ssem, recv_sem=rsem,
            device_id=dev, device_id_type=pl.DeviceIdType.MESH,
        )

    def got(ref, rsem):
        rc(ref, ref, rsem, rsem, (s, mate)).wait_recv()

    def sent(ref, ssem):
        rc(ref, ref, ssem, ssem, (s, mate)).wait_send()

    loads = [
        pltpu.make_async_copy(src, dst, in_sem.at[i])
        for i, (src, dst) in enumerate(
            ((hid_hbm, hid), (cot_hbm, cot), (tok_hbm, tok), (tgt_hbm, tgt), (scale_hbm, scale), (slab_hbm, slab))
        )
    ]
    for load in loads:
        load.start()

    bar = pltpu.get_barrier_semaphore()
    for r in range(1, S):
        pl.semaphore_signal(bar, inc=1, device_id=((s + r) % S, v), device_id_type=pl.DeviceIdType.MESH)
    for r in range(1, V):
        pl.semaphore_signal(bar, inc=1, device_id=(s, (v + r) % V), device_id_type=pl.DeviceIdType.MESH)
    for load in loads[:5]:
        load.wait()
    tid_tx[...] = jnp.broadcast_to(tok[...], tid_tx.shape)
    ids[s] = jnp.broadcast_to(tok[...], tid_tx.shape)
    pl.semaphore_wait(bar, S + V - 2)

    def z_send(k):
        b = z - k

        @pl.when((z < Z - 1) & (b >= 0))
        def _():
            rc(hid if k == 0 else zg.at[b], zg.at[b], zr_s.at[k], zr_r.at[k], (s, v + 2)).start()

        d = z + k

        @pl.when((z > 0) & (d <= Z - 1))
        def _():
            rc(hid if k == 0 else zg.at[d], zg.at[d], zl_s.at[k], zl_r.at[k], (s, v - 2)).start()

    def plane_send(b, src):
        @pl.when(b != s)
        def _():
            rc(src, hq.at[s], pl_s.at[b], pl_r.at[s], (b, v)).start()

        @pl.when(b == s)
        def _():
            rc(src, hm.at[s], mt_s.at[s], mt_r.at[s], (s, mate)).start()
            hq[s] = src[...]

    z_send(0)
    plane_send(z, hid)

    @pl.when(s != z)
    def _():
        rc(cot, cq.at[s], cp_s, cp_r.at[s], (z, v)).start()

    for r in range(1, S):
        t = (s + r) % S
        rc(tid_tx, ids.at[s], id_s.at[r - 1], id_r.at[s], (t, v)).start()

    for k in range(Z - 1):
        b = z - 1 - k
        d = z + 1 + k

        @pl.when(b >= 0)
        def _():
            got(zg.at[b], zr_r.at[k])

        @pl.when(d <= Z - 1)
        def _():
            got(zg.at[d], zl_r.at[k])

        if k + 1 < Z - 1:
            z_send(k + 1)

        @pl.when(b >= 0)
        def _():
            plane_send(b, zg.at[b])

        @pl.when(d <= Z - 1)
        def _():
            plane_send(d, zg.at[d])

    for r in range(1, S):
        t = (s + r) % S
        got(hq.at[t], pl_r.at[t])
        rc(hq.at[t], hm.at[t], mt_s.at[t], mt_r.at[t], (s, mate)).start()

    def assemble(full, mine, other, t):
        cols = slice(t % 2 * T, (t % 2 + 1) * T)
        full[t // 2, pl.ds(pl.multiple_of(c * W, 16), W), cols] = mine[t]
        full[t // 2, pl.ds(pl.multiple_of((1 - c) * W, 16), W), cols] = other[t]

    for t in range(S):
        got(hm.at[t], mt_r.at[t])
        assemble(h, hq, hm, t)
    loads[5].wait()

    def forward(src, t):
        @pl.when((z >= s) & (z < Z - 1))
        def _():
            rc(src, cq.at[t], cr_s.at[t], cz_r.at[t], (s, v + 2)).start()

        @pl.when((z <= s) & (z > 0))
        def _():
            rc(src, cq.at[t], cl_s.at[t], cz_r.at[t], (s, v - 2)).start()

        rc(src, cm.at[t], cm_s.at[t], cm_r.at[t], (s, mate)).start()

    @pl.when(z == s)
    def _():
        cq[s] = cot[...]
        forward(cot, s)
        for r in range(1, S):
            t = (s + r) % S
            got(cq.at[t], cp_r.at[t])
            forward(cq.at[t], t)

    low, high = slice(0, half), slice(half, R)

    def logits(p, last):
        def logit_tile(j, carry):
            rows = pl.ds(pl.multiple_of(j * tile, tile), tile)
            part = jnp.dot(slab[rows, :], h[p], preferred_element_type=f32)
            for m in range(2):
                snd[2 * p + m, rows, :] = encode(part[:, m * T:(m + 1) * T])
            if last:
                own[rows, :] = jnp.where(s % 2 == 0, part[:, :T], part[:, T:])
            return carry

        lax.fori_loop(0, R // tile, logit_tile, 0)

    def logit_send(n, t, slot, part, to):
        rc(snd.at[t, part], rcv.at[slot, part], rs_s.at[n], rs_r.at[n], (to, v)).start()

    def logit_got(n, slot, part):
        got(rcv.at[slot, part], rs_r.at[n])

    def relay(t, part):
        def relay_tile(j, carry):
            rows = pl.ds(pl.multiple_of(part.start + j * tile, tile), tile)
            snd[t, rows, :] = encode(decode(snd[t, rows, :]) + decode(rcv[2, rows, :]))
            return carry

        lax.fori_loop(0, half // tile, relay_tile, 0)

    other = 1 - s // 2
    logits(other, False)
    logit_send(0, far, 2, low, nx)
    logit_send(1, far, 2, high, ny)
    logit_send(2, ny, 1, high, ny)
    logits(s // 2, True)
    logit_send(3, nx, 0, low, nx)
    logit_got(0, 2, low)
    relay(ny, low)
    logit_send(4, ny, 1, low, ny)
    logit_got(1, 2, high)
    relay(nx, high)
    logit_send(5, nx, 0, high, nx)

    apart = jnp.abs(z - s)

    def pass_cot(distance):
        @pl.when(apart == distance)
        def _():
            for r in range(S):
                t = (s + r) % S
                got(cq.at[t], cz_r.at[t])
                forward(cq.at[t], t)

    pass_cot(1)
    logit_got(2, 1, high)
    logit_got(3, 0, low)
    logit_got(4, 1, low)
    logit_got(5, 0, high)
    soft = 128
    target = tgt[...]

    def row_ids(j, n, width):
        return v * R + j * n + lax.broadcasted_iota(jnp.int32, (n, width), 0)

    def soft_tile(j, carry):
        total, pick = carry
        rows = pl.ds(pl.multiple_of(j * soft, soft), soft)
        raw = own[rows, :] + decode(rcv[0, rows, :]) + decode(rcv[1, rows, :])
        capped = logit_cap * jnp.tanh(raw / logit_cap)
        e = jnp.exp(capped)
        cap[rows, :] = capped
        ex[rows, :] = e
        hit = row_ids(j, soft, T) == target
        total = total + jnp.sum(e, axis=0, keepdims=True)
        pick = pick + jnp.sum(jnp.where(hit, capped, 0.0), axis=0, keepdims=True)
        return total, pick

    zero = jnp.zeros((1, T), f32)
    total, pick = lax.fori_loop(0, R // soft, soft_tile, (zero, zero))
    stat_tx[0:8, :] = jnp.broadcast_to(total, (8, T))
    stat_tx[8:16, :] = jnp.broadcast_to(pick, (8, T))
    for r in range(1, V):
        rc(stat_tx, stat_rx.at[v], st_s.at[r - 1], st_r.at[v], (s, (v + r) % V)).start()
    stat_rx[v] = stat_tx[...]
    pass_cot(2)
    for r in range(1, V):
        u = (v + r) % V
        got(stat_rx.at[u], st_r.at[u])
    sums = stat_rx[0]
    for u in range(1, V):
        sums = sums + stat_rx[u]
    total = sums[0:1, :]
    loss[...] = jnp.log(total) - sums[8:9, :]
    gain = scale[...]

    def grad_tile(j, carry):
        rows = pl.ds(pl.multiple_of(j * soft, soft), soft)
        capped = cap[rows, :]
        hit = (row_ids(j, soft, T) == target).astype(f32)
        slope = 1.0 - (capped / logit_cap) ** 2
        dl[s, rows, :] = (gain * (ex[rows, :] / total - hit) * slope).astype(bf16)
        return carry

    lax.fori_loop(0, R // soft, grad_tile, 0)

    def grad_send(n, t, part, to):
        block = dl.at[t, part]
        rc(block, block, ag_s.at[n], ag_r.at[n], (to, v)).start()

    def grad_got(n, t, part):
        got(dl.at[t, part], ag_r.at[n])

    grad_send(0, s, high, nx)
    grad_send(1, s, low, ny)
    grad_send(2, s, low, nx)
    grad_send(3, s, high, ny)

    def term(t):
        g = lax.dot_general(
            dl[t], slab[...], (((0,), (0,)), ((), ())), preferred_element_type=f32
        )

        gt[t] = g.T
        give = gt.at[t, pl.ds(pl.multiple_of((1 - c) * W, 16), W)]
        rc(give, px_rx.at[t], px_s.at[t], px_r.at[t], (s, mate)).start()

    def fin_send(q, src):
        @pl.when(q != z)
        def _():
            rc(src, fin.at[z], f_s.at[q], f_r.at[z], (s, 2 * q + c)).start()

        @pl.when(q == z)
        def _():
            fin[z] = src[...]

    def pass_on(t, local):
        got(px_rx.at[t], px_r.at[t])
        kept = gt[t, pl.ds(pl.multiple_of(c * W, 16), W), :]
        gs[t] = (kept + px_rx[t]).astype(bf16)
        if local:
            fin_send(s, gs.at[t])
        else:
            rc(gs.at[t], zr.at[s], g_s.at[t], g_r.at[s], (t, v)).start()

    term(s)
    grad_got(1, ny, low)
    grad_send(4, ny, low, nx)
    grad_got(0, nx, high)
    grad_send(5, nx, high, ny)
    pass_on(s, True)
    grad_got(2, nx, low)
    term(nx)
    grad_got(3, ny, high)
    term(ny)
    pass_on(nx, False)
    pass_on(ny, False)
    grad_got(4, far, low)
    grad_got(5, far, high)
    term(far)

    def fin_pass(q):
        got(zr.at[q], g_r.at[q])
        fin_send(q, zr.at[q])

    fin_pass(nx)
    fin_pass(ny)
    pass_on(far, False)
    for distance in range(3, Z):
        pass_cot(distance)
    for t in range(S):
        got(cm.at[t], cm_r.at[t])
        assemble(cf, cq, cm, t)

    for r in range(1, S):
        t = (s + r) % S
        got(ids.at[t], id_r.at[t])
    every = jnp.concatenate([ids[t][0:1, :] for t in range(S)], axis=1)
    root = math.sqrt(Q * S)

    def tied_tile(j, carry):
        rows = pl.ds(pl.multiple_of(j * tile, tile), tile)
        onehot = (row_ids(j, tile, S * T) == every).astype(f32).astype(bf16)
        head, embed = 0.0, 0.0
        for p in range(S // 2):
            lhs = jnp.concatenate([dl[2 * p, rows, :], dl[2 * p + 1, rows, :]], axis=1)
            head = head + over_tokens(lhs, h[p])
            embed = embed + over_tokens(onehot[:, 2 * p * T:2 * (p + 1) * T], cf[p])
        tied[rows, :] = (head + embed * root).astype(bf16)
        return carry

    middle = R // tile // 2
    lax.fori_loop(0, middle, tied_tile, 0)
    fin_pass(far)
    lax.fori_loop(middle, R // tile, tied_tile, 0)

    for r in range(1, Z):
        u = (z + r) % Z
        got(fin.at[u], f_r.at[u])
    acc = fin[0].astype(f32)
    for u in range(1, Z):
        acc = acc + fin[u].astype(f32)
    hgrad[...] = acc.astype(bf16)

    for k in range(Z - 1):
        @pl.when((z < Z - 1) & (z - k >= 0))
        def _():
            sent(hid, zr_s.at[k])

        @pl.when((z > 0) & (z + k <= Z - 1))
        def _():
            sent(hid, zl_s.at[k])
    for b in range(S):
        @pl.when(b != s)
        def _():
            sent(hid, pl_s.at[b])
            sent(gs.at[b], g_s.at[b])
        sent(hid, mt_s.at[b])
        sent(cot, cm_s.at[b])
        sent(px_rx.at[b], px_s.at[b])

        @pl.when((z >= s) & (z < Z - 1))
        def _():
            sent(cot, cr_s.at[b])

        @pl.when((z <= s) & (z > 0))
        def _():
            sent(cot, cl_s.at[b])
    for q in range(Z):
        @pl.when(q != z)
        def _():
            sent(gs.at[0], f_s.at[q])

    @pl.when(s != z)
    def _():
        sent(cot, cp_s)
    for r in range(1, S):
        sent(tid_tx, id_s.at[r - 1])
    for n in range(6):
        sent(snd.at[0, low], rs_s.at[n])
        sent(dl.at[0, low], ag_s.at[n])
    for r in range(1, V):
        sent(stat_tx, st_s.at[r - 1])


def put_out(loss, hgrad, tied, loss_out, hgrad_out, tied_out, sems):
    moves = [
        pltpu.make_async_copy(src, dst, sems.at[i])
        for i, (src, dst) in enumerate(((tied, tied_out), (hgrad, hgrad_out), (loss, loss_out)))
    ]
    for move in moves:
        move.start()
    for move in moves:
        move.wait()


def fused(hidden, slab, token_ids, target_ids, input_cot, loss_grad):
    S = lax.axis_size("section")
    V = lax.axis_size("vocab")
    Z = V // 2
    T, W = hidden.shape
    R, Q = slab.shape
    vm = pltpu.VMEM
    dma = pltpu.SemaphoreType.DMA
    half = vm((S, W, T), bf16)
    both = vm((S // 2, Q, 2 * T), bf16)
    scratch = [
        vm((W, T), bf16), vm((W, T), bf16),
        vm((1, T), jnp.int32), vm((1, T), jnp.int32), vm((1, T), f32),
        vm((R, Q), bf16), half, half, half, both,
        vm((S, R, T), jnp.int16), vm((3, R, T), jnp.int16), vm((R, T), f32),
        half, half, both, vm((S, 8, T), jnp.int32), vm((8, T), jnp.int32),
        vm((R, T), f32), vm((R, T), f32), vm((16, T), f32), vm((V, 16, T), f32),
        vm((S, R, T), bf16), vm((S, Q, T), f32), vm((S, W, T), f32), half, half, vm((Z, W, T), bf16),
        dma((6,)), dma((Z,)), dma((Z,)), dma((Z,)), dma((Z,)),
        dma((S,)), dma((S,)), dma((S,)), dma((S,)), dma, dma((S,)),
        dma((S,)), dma((S,)), dma((S,)), dma((S,)), dma((S,)), dma((S,)), dma((S,)),
        dma((6,)), dma((6,)), dma((V,)), dma((V,)), dma((6,)), dma((6,)),
        dma((S,)), dma((S,)), dma((S,)), dma((S,)), dma((Z,)), dma((Z,)),
    ]
    block = pl.BlockSpec(memory_space=vm)
    anywhere = pl.BlockSpec(memory_space=pl.ANY)
    far_memory = pl.BlockSpec(memory_space=pltpu.HBM)
    results = pl.pallas_call(
        functools.partial(fused_kernel, (S, V)),
        out_shape=(
            jax.ShapeDtypeStruct((1, T), f32),
            jax.ShapeDtypeStruct((W, T), bf16),
            jax.ShapeDtypeStruct((R, Q), bf16),
        ),
        in_specs=[far_memory] * 6,
        out_specs=(block, block, block),
        scratch_shapes=scratch,
        compiler_params=pltpu.CompilerParams(
            collective_id=0, has_side_effects=True, vmem_limit_bytes=48 * 2**20
        ),
        name="fused",
    )(
        *(
            pltpu.with_memory_space_constraint(x, pltpu.HBM)
            for x in (
                hidden.T, input_cot.T, slab,
                token_ids.reshape(1, T), target_ids.reshape(1, T), loss_grad.reshape(1, T),
            )
        )
    )
    loss, hgrad, tied = pl.pallas_call(
        put_out,
        out_shape=tuple(jax.ShapeDtypeStruct(x.shape, x.dtype) for x in results),
        in_specs=[block] * 3,
        out_specs=(anywhere,) * 3,
        scratch_shapes=[dma((3,))],
        compiler_params=pltpu.CompilerParams(vmem_limit_bytes=8 * 2**20),
        name="put_out",
    )(*results)
    return loss.reshape(T), hgrad.T, tied


def from_partner(block, axis, stride):
    count = lax.axis_size(axis)
    route = []
    for low in range(count):
        high = low | 1 << stride
        if high != low and high < count:
            route += [(low, high), (high, low)]
    return lax.ppermute(block, axis, route)


def left_product(left_side, right_side):
    return lax.dot_general(
        left_side, right_side, (((0,), (0,)), ((), ())), preferred_element_type=jnp.float32
    )


def local_parts(raw_logits, targets, columns):
    capped = logit_cap * jnp.tanh(raw_logits / logit_cap)
    exp_logits = jnp.exp(capped)
    target_hit = (targets[:, None] == columns[None, :]).astype(jnp.float32)
    local_total = jnp.sum(exp_logits, axis=1)
    local_pick = jnp.sum(target_hit * capped, axis=1)
    return (capped, exp_logits, target_hit, local_total, local_pick)


def finish(capped, exp_logits, target_hit, exp_total, picked, scales):
    token_loss = jnp.log(exp_total) - picked
    slope = 1.0 - (capped / logit_cap) ** 2
    dlogit = (scales[:, None] * (exp_logits / exp_total[:, None] - target_hit) * slope).astype(
        jnp.bfloat16
    )
    return (token_loss, dlogit)


def general(hidden, slab, token_ids, target_ids, input_cot, loss_grad):
    rows_here = slab.shape[0]
    quarter_width = slab.shape[1]
    sections = lax.axis_size("section")
    shards = lax.axis_size("vocab")
    model_width = quarter_width * sections
    own_tokens = hidden.shape[0]
    share_width = hidden.shape[1]
    full_hidden, full_cot = (
        lax.all_gather(hidden, "vocab", axis=1, tiled=True),
        lax.all_gather(input_cot, "vocab", axis=1, tiled=True),
    )
    hidden_part, cot_part = (
        lax.all_to_all(full_hidden, "section", split_axis=1, concat_axis=0, tiled=True),
        lax.all_to_all(full_cot, "section", split_axis=1, concat_axis=0, tiled=True),
    )
    partial_value = lax.dot_general(
        hidden_part, slab, (((1,), (1,)), ((), ())), preferred_element_type=jnp.float32
    )
    columns = lax.axis_index("vocab") * rows_here + jnp.arange(rows_here, dtype=jnp.int32)
    raw_logits = lax.psum_scatter(partial_value, "section", scatter_dimension=0, tiled=True)
    capped, exp_logits, target_hit, local_total, local_pick = local_parts(
        raw_logits, target_ids, columns
    )
    exp_total, picked = lax.psum((local_total, local_pick), "vocab")
    token_loss, dlogit = finish(capped, exp_logits, target_hit, exp_total, picked, loss_grad)
    all_ids = lax.all_gather(token_ids, "section", axis=0, tiled=True)
    all_dlogit = lax.all_gather(dlogit, "section", axis=0, tiled=True)
    total_tokens = all_dlogit.shape[0]
    blocks = shards // sections
    narrow = share_width // sections
    arranged_slab = slab.reshape(rows_here, blocks, sections, narrow)
    term = jnp.einsum(
        "tv,vkrw->trkw", all_dlogit, arranged_slab, preferred_element_type=jnp.float32
    )
    term = term.reshape(total_tokens, shards * narrow)
    piece = lax.psum_scatter(term, "vocab", scatter_dimension=1, tiled=True).astype(jnp.bfloat16)
    slots = lax.all_to_all(piece, "section", split_axis=0, concat_axis=0, tiled=True).reshape(
        sections, own_tokens, narrow
    )
    base_bit = blocks.bit_length() - 1
    rank_high = lax.axis_index("vocab") // blocks
    for level in range(sections.bit_length() - 1):
        span = 1 << level
        shaped = slots.reshape(sections // (2 * span), 2, span, own_tokens, narrow)
        mine_bit = rank_high // span % 2
        lower = shaped[:, 0]
        upper = shaped[:, 1]
        keep = jnp.where(mine_bit == 0, lower, upper)
        outgoing = jnp.where(mine_bit == 0, upper, lower)
        incoming = from_partner(outgoing, "vocab", base_bit + level)
        first = jnp.where(mine_bit == 0, keep, incoming)
        second = jnp.where(mine_bit == 0, incoming, keep)
        slots = jnp.stack([first, second], axis=1).reshape(sections, own_tokens, narrow)
    hidden_grad = jnp.transpose(slots, (1, 0, 2)).reshape(own_tokens, sections * narrow)
    onehot = (all_ids[:, None] == columns[None, :]).astype(jnp.bfloat16)
    embed_scale = math.sqrt(model_width)
    tied_grad = left_product(all_dlogit, hidden_part) + left_product(onehot, cot_part) * embed_scale
    return (token_loss, hidden_grad, tied_grad.astype(jnp.bfloat16))


def on_device(hidden, slab, token_ids, target_ids, input_cot, loss_grad):
    sections = lax.axis_size("section")
    shards = lax.axis_size("vocab")
    fits = (
        sections == 4
        and shards == 2 * sections
        and hidden.shape[0] % 128 == 0
        and slab.shape[0] % 256 == 0
    )
    step = fused if fits else general
    return step(hidden, slab, token_ids, target_ids, input_cot, loss_grad)


def solution(mesh):
    placed = (
        P("section", "vocab"),
        P("vocab", "section"),
        P("section"),
        P("section"),
        P("section", "vocab"),
        P("section"),
    )
    return jax.shard_map(
        on_device,
        mesh=mesh,
        in_specs=placed,
        out_specs=(P("section"), P("section", "vocab"), P("vocab", "section")),
        check_vma=False,
    )
```

```python
import functools
import math

import jax
import jax.numpy as jnp
from jax import lax
from jax.experimental import pallas as pl
from jax.experimental.pallas import tpu as pltpu
from jax.sharding import PartitionSpec as P

logit_cap = 30.0
code_knee = 16.0
code_top = 32767.0
f32 = jnp.float32
bf16 = jnp.bfloat16


steps = 2
shares = 2


def encode(x):
    y = x / (jnp.abs(x) + code_knee) * code_top
    return jnp.floor(y + 0.5).astype(jnp.int32).astype(jnp.int16)


def decode(code):
    y = code.astype(jnp.int32).astype(f32) * (1.0 / code_top)
    return code_knee * y / (1.0 - jnp.abs(y))


def over_tokens(left, right):
    return lax.dot_general(
        left, right, (((1,), (1,)), ((), ())), preferred_element_type=jnp.float32
    )


def fused_kernel(
    dims, hid_hbm, cot_hbm, slab_hbm, tok_hbm, tgt_hbm, scale_hbm, loss, hgrad, tied,
    hid, cot, tok, tgt, scale,
    slab, zg, hq, hm, h, snd, rcv, own, cq, cm, cf, ids, tid_tx, cd, stat_tx, stat_rx,
    info, dl, gt, px_rx, gs, zr, fin,
    in_sem, zr_s, zr_r, zl_s, zl_r, pl_s, pl_r, mt_s, mt_r, cp_s, cp_r, cr_s, cl_s, cz_r,
    cm_s, cm_r, id_s, id_r, in_s, in_r, rs_s, rs_r, st_s, st_r, ag_s, ag_r, px_s, px_r, g_s, g_r, f_s, f_r,
):
    S, V = dims
    Z = V // 2
    W, T = hid.shape
    R, Q = slab.shape
    span = R // steps
    half = span // 2
    s = lax.axis_index("section")
    v = lax.axis_index("vocab")
    z = v // 2
    c = v % 2
    mate = z * 2 + 1 - c
    nx, ny, far = s ^ 1, s ^ 2, s ^ 3
    tile = 256

    def rc(src, dst, ssem, rsem, dev):
        return pltpu.make_async_remote_copy(
            src_ref=src, dst_ref=dst, send_sem=ssem, recv_sem=rsem,
            device_id=dev, device_id_type=pl.DeviceIdType.MESH,
        )

    def got(ref, rsem):
        rc(ref, ref, rsem, rsem, (s, mate)).wait_recv()

    def sent(ref, ssem):
        rc(ref, ref, ssem, ssem, (s, mate)).wait_send()

    loads = [
        pltpu.make_async_copy(src, dst, in_sem.at[i])
        for i, (src, dst) in enumerate(
            ((hid_hbm, hid), (cot_hbm, cot), (tok_hbm, tok), (tgt_hbm, tgt), (scale_hbm, scale), (slab_hbm, slab))
        )
    ]
    for load in loads:
        load.start()

    bar = pltpu.get_barrier_semaphore()
    for r in range(1, S):
        pl.semaphore_signal(bar, inc=1, device_id=((s + r) % S, v), device_id_type=pl.DeviceIdType.MESH)
    for r in range(1, V):
        pl.semaphore_signal(bar, inc=1, device_id=(s, (v + r) % V), device_id_type=pl.DeviceIdType.MESH)
    for load in loads[:5]:
        load.wait()
    both_ids = jnp.concatenate([jnp.broadcast_to(x[...], (4, T)) for x in (tok, tgt)], axis=0)
    tid_tx[...] = both_ids
    ids[s] = both_ids
    pl.semaphore_wait(bar, S + V - 2)

    piece = W // shares
    slices = [slice(f * piece, (f + 1) * piece) for f in range(shares)]

    def z_send(k, f):
        part = slices[f]
        n = k * shares + f
        b = z - k

        @pl.when((z < Z - 1) & (b >= 0))
        def _():
            src = hid.at[part] if k == 0 else zg.at[b, part]
            rc(src, zg.at[b, part], zr_s.at[n], zr_r.at[n], (s, v + 2)).start()

        d = z + k

        @pl.when((z > 0) & (d <= Z - 1))
        def _():
            src = hid.at[part] if k == 0 else zg.at[d, part]
            rc(src, zg.at[d, part], zl_s.at[n], zl_r.at[n], (s, v - 2)).start()

    def plane_send(b, src, f):
        part = slices[f]

        @pl.when(b != s)
        def _():
            rc(src, hq.at[s, part], pl_s.at[b * shares + f], pl_r.at[s * shares + f], (b, v)).start()

        @pl.when(b == s)
        def _():
            n = s * shares + f
            rc(src, hm.at[s, part], mt_s.at[n], mt_r.at[n], (s, mate)).start()
            hq[s, part] = src[...]

    for f in range(shares):
        z_send(0, f)
    for f in range(shares):
        plane_send(z, hid.at[slices[f]], f)

    @pl.when(s != z)
    def _():
        rc(cot, cq.at[s], cp_s, cp_r.at[s], (z, v)).start()

    for r in range(1, S):
        t = (s + r) % S
        rc(tid_tx, ids.at[s], id_s.at[r - 1], id_r.at[s], (t, v)).start()

    for k in range(Z - 1):
        b = z - 1 - k
        d = z + 1 + k
        for f in range(shares):
            part = slices[f]
            n = k * shares + f

            @pl.when(b >= 0)
            def _():
                got(zg.at[b, part], zr_r.at[n])

            @pl.when(d <= Z - 1)
            def _():
                got(zg.at[d, part], zl_r.at[n])

            if k + 1 < Z - 1:
                z_send(k + 1, f)

            @pl.when(b >= 0)
            def _():
                plane_send(b, zg.at[b, part], f)

            @pl.when(d <= Z - 1)
            def _():
                plane_send(d, zg.at[d, part], f)

    def forward(src, t):
        @pl.when((z >= s) & (z < Z - 1))
        def _():
            rc(src, cq.at[t], cr_s.at[t], cz_r.at[t], (s, v + 2)).start()

        @pl.when((z <= s) & (z > 0))
        def _():
            rc(src, cq.at[t], cl_s.at[t], cz_r.at[t], (s, v - 2)).start()

        rc(src, cm.at[t], cm_s.at[t], cm_r.at[t], (s, mate)).start()

    @pl.when(z == s)
    def _():
        cq[s] = cot[...]
        forward(cot, s)
        for r in range(1, S):
            t = (s + r) % S
            got(cq.at[t], cp_r.at[t])
            forward(cq.at[t], t)

    apart = jnp.abs(z - s)

    def pass_cot(distance, first, last):
        @pl.when(apart == distance)
        def _():
            for r in range(first, last):
                t = (s + r) % S
                got(cq.at[t], cz_r.at[t])
                forward(cq.at[t], t)

    for f in range(shares):
        for r in range(1, S):
            t = s ^ r
            n = t * shares + f
            got(hq.at[t, slices[f]], pl_r.at[n])
            rc(hq.at[t, slices[f]], hm.at[t, slices[f]], mt_s.at[n], mt_r.at[n], (s, mate)).start()

    def assemble(full, mine, other, t):
        cols = slice(t % 2 * T, (t % 2 + 1) * T)
        full[t // 2, pl.ds(pl.multiple_of(c * W, 16), W), cols] = mine[t]
        full[t // 2, pl.ds(pl.multiple_of((1 - c) * W, 16), W), cols] = other[t]

    for t in range(S):
        for f in range(shares):
            got(hm.at[t, slices[f]], mt_r.at[t * shares + f])
        assemble(h, hq, hm, t)
    loads[5].wait()

    low = [slice(k * span, k * span + half) for k in range(steps)]
    high = [slice(k * span + half, (k + 1) * span) for k in range(steps)]
    other = 1 - s // 2
    even = s % 2 == 0

    def logits(k):
        def logit_tile(j, carry):
            rows = pl.ds(pl.multiple_of(k * span + j * tile, tile), tile)
            part = jnp.dot(slab[rows, :], h[other], preferred_element_type=f32)
            for m in range(2):
                snd[2 * other + m, rows, :] = encode(part[:, m * T:(m + 1) * T])
            part = jnp.dot(slab[rows, :], h[s // 2], preferred_element_type=f32)
            own[rows, :] = jnp.where(even, part[:, :T], part[:, T:])
            snd[nx, rows, :] = encode(jnp.where(even, part[:, T:], part[:, :T]))
            return carry

        lax.fori_loop(0, span // tile, logit_tile, 0)

    def logit_send(n, t, slot, part, to):
        rc(snd.at[t, part], rcv.at[slot, part], rs_s.at[n], rs_r.at[n], (to, v)).start()

    def logit_got(n, slot, part):
        got(rcv.at[slot, part], rs_r.at[n])

    def relay(t, part):
        def relay_tile(j, carry):
            rows = pl.ds(pl.multiple_of(part.start + j * tile, tile), tile)
            snd[t, rows, :] = encode(decode(snd[t, rows, :]) + decode(rcv[2, rows, :]))
            return carry

        lax.fori_loop(0, half // tile, relay_tile, 0)

    def logit_start(k):
        logit_send(6 * k, far, 2, low[k], nx)
        logit_send(6 * k + 1, far, 2, high[k], ny)
        logit_send(6 * k + 2, nx, 0, low[k], nx)
        logit_send(6 * k + 3, ny, 1, high[k], ny)

    def logit_relay(k):
        logit_got(6 * k, 2, low[k])
        relay(ny, low[k])
        logit_send(6 * k + 4, ny, 1, low[k], ny)
        logit_got(6 * k + 1, 2, high[k])
        relay(nx, high[k])
        logit_send(6 * k + 5, nx, 0, high[k], nx)

    soft = 128
    target = tgt[...]
    unit = logit_cap / code_top

    def row_ids(j, n, width):
        return v * R + j * n + lax.broadcasted_iota(jnp.int32, (n, width), 0)

    def softmax_sums(k, sums):
        logit_got(6 * k + 2, 0, low[k])
        logit_got(6 * k + 3, 1, high[k])
        logit_got(6 * k + 4, 1, low[k])
        logit_got(6 * k + 5, 0, high[k])

        def soft_tile(j, carry):
            total, pick = carry
            rows = pl.ds(pl.multiple_of(j * soft, soft), soft)
            raw = own[rows, :] + decode(rcv[0, rows, :]) + decode(rcv[1, rows, :])
            bent = jnp.tanh(raw / logit_cap)
            code = jnp.floor(bent * code_top + 0.5)
            cd[s, rows, :] = code.astype(jnp.int32).astype(jnp.int16)
            hit = row_ids(j, soft, T) == target
            total = total + jnp.sum(jnp.exp(code * unit), axis=0, keepdims=True)
            pick = pick + jnp.sum(jnp.where(hit, logit_cap * bent, 0.0), axis=0, keepdims=True)
            return total, pick

        count = span // soft
        return lax.fori_loop(k * count, (k + 1) * count, soft_tile, sums)

    def code_send(n, t, part, to):
        block = cd.at[t, part]
        rc(block, block, ag_s.at[n], ag_r.at[n], (to, v)).start()

    def code_got(n, t, part):
        got(cd.at[t, part], ag_r.at[n])

    def code_start(k):
        code_send(6 * k, s, high[k], nx)
        code_send(6 * k + 1, s, low[k], ny)
        code_send(6 * k + 2, s, low[k], nx)
        code_send(6 * k + 3, s, high[k], ny)

    def code_relay(k):
        code_got(6 * k + 1, ny, low[k])
        code_send(6 * k + 4, ny, low[k], nx)
        code_got(6 * k, nx, high[k])
        code_send(6 * k + 5, nx, high[k], ny)

    def info_got(t):
        got(info.at[t], in_r.at[t])

    def grad(t, k):
        scale_row = info[t][0:1, :]
        gain_row = info[t][1:2, :]
        target_row = ids[t][4:5, :]

        def grad_tile(j, carry):
            rows = pl.ds(pl.multiple_of(j * soft, soft), soft)
            code = cd[t, rows, :].astype(jnp.int32).astype(f32)
            hit = row_ids(j, soft, T) == target_row
            slope = 1.0 - (code * (1.0 / code_top)) ** 2
            away = jnp.exp(code * unit) * scale_row - jnp.where(hit, gain_row, 0.0)
            dl[t, rows, :] = (away * slope).astype(bf16)
            return carry

        count = span // soft
        lax.fori_loop(k * count, (k + 1) * count, grad_tile, 0)

    zero = jnp.zeros((1, T), f32)
    logits(0)
    logit_start(0)
    logits(1)
    pass_cot(1, 0, 2)
    logit_relay(0)
    logit_start(1)
    pass_cot(1, 2, S)
    pass_cot(2, 0, 2)
    sums = softmax_sums(0, (zero, zero))
    pass_cot(2, 2, S)
    logit_relay(1)
    code_start(0)
    total, pick = softmax_sums(1, sums)
    stat_tx[0:8, :] = jnp.broadcast_to(total, (8, T))
    stat_tx[8:16, :] = jnp.broadcast_to(pick, (8, T))
    for r in range(1, V):
        rc(stat_tx, stat_rx.at[v], st_s.at[r - 1], st_r.at[v], (s, (v + r) % V)).start()
    stat_rx[v] = stat_tx[...]
    for r in range(1, S):
        t = (s + r) % S
        got(ids.at[t], id_r.at[t])
    code_relay(0)
    for r in range(1, V):
        u = (v + r) % V
        got(stat_rx.at[u], st_r.at[u])
    sums = stat_rx[0]
    for u in range(1, V):
        sums = sums + stat_rx[u]
    total = sums[0:1, :]
    loss[...] = jnp.log(total) - sums[8:9, :]
    gain = scale[...]
    info[s] = jnp.concatenate(
        [gain / total, jnp.broadcast_to(gain, (7, T))], axis=0
    )
    for r in range(1, S):
        t = s ^ r
        rc(info.at[s], info.at[s], in_s.at[r - 1], in_r.at[s], (t, v)).start()
    code_start(1)

    def term(t):
        g = lax.dot_general(
            dl[t], slab[...], (((0,), (0,)), ((), ())), preferred_element_type=f32
        )

        gt[t] = g.T
        give = gt.at[t, pl.ds(pl.multiple_of((1 - c) * W, 16), W)]
        rc(give, px_rx.at[t], px_s.at[t], px_r.at[t], (s, mate)).start()

    def fin_send(q, src):
        @pl.when(q != z)
        def _():
            rc(src, fin.at[z], f_s.at[q], f_r.at[z], (s, 2 * q + c)).start()

        @pl.when(q == z)
        def _():
            fin[z] = src[...]

    def pass_on(t, local):
        got(px_rx.at[t], px_r.at[t])
        kept = gt[t, pl.ds(pl.multiple_of(c * W, 16), W), :]
        gs[t] = (kept + px_rx[t]).astype(bf16)
        if local:
            fin_send(s, gs.at[t])
        else:
            rc(gs.at[t], zr.at[s], g_s.at[t], g_r.at[s], (t, v)).start()

    for k in range(steps):
        grad(s, k)
    term(s)
    for t, n in ((nx, 2), (ny, 3)):
        info_got(t)
    code_got(2, nx, low[0])
    grad(nx, 0)
    pass_on(s, True)
    code_got(3, ny, high[0])
    grad(ny, 0)
    code_relay(1)
    info_got(far)
    code_got(4, far, low[0])
    code_got(5, far, high[0])
    grad(far, 0)
    code_got(8, nx, low[1])
    grad(nx, 1)
    term(nx)
    code_got(9, ny, high[1])
    grad(ny, 1)
    term(ny)
    pass_on(nx, False)
    pass_on(ny, False)
    code_got(10, far, low[1])
    code_got(11, far, high[1])
    grad(far, 1)
    term(far)

    def fin_pass(q):
        got(zr.at[q], g_r.at[q])
        fin_send(q, zr.at[q])

    for distance in range(3, Z):
        pass_cot(distance, 0, S)
    for t in range(S):
        got(cm.at[t], cm_r.at[t])
        assemble(cf, cq, cm, t)
    every = jnp.concatenate([ids[t][0:1, :] for t in range(S)], axis=1)
    root = math.sqrt(Q * S)

    def tied_tile(j, carry):
        rows = pl.ds(pl.multiple_of(j * tile, tile), tile)
        onehot = (row_ids(j, tile, S * T) == every).astype(f32).astype(bf16)
        head, embed = 0.0, 0.0
        for p in range(S // 2):
            lhs = jnp.concatenate([dl[2 * p, rows, :], dl[2 * p + 1, rows, :]], axis=1)
            head = head + over_tokens(lhs, h[p])
            embed = embed + over_tokens(onehot[:, 2 * p * T:2 * (p + 1) * T], cf[p])
        tied[rows, :] = (head + embed * root).astype(bf16)
        return carry

    tiles = R // tile
    marks = [0, tiles // 8, tiles // 4, tiles * 5 // 8, tiles]
    lax.fori_loop(marks[0], marks[1], tied_tile, 0)
    pass_on(far, False)
    lax.fori_loop(marks[1], marks[2], tied_tile, 0)
    fin_pass(nx)
    fin_pass(ny)
    lax.fori_loop(marks[2], marks[3], tied_tile, 0)
    fin_pass(far)
    lax.fori_loop(marks[3], marks[4], tied_tile, 0)
    for r in range(1, Z):
        u = (z + r) % Z
        got(fin.at[u], f_r.at[u])
    acc = fin[0].astype(f32)
    for u in range(1, Z):
        acc = acc + fin[u].astype(f32)
    hgrad[...] = acc.astype(bf16)

    for k in range(Z - 1):
        for f in range(shares):
            @pl.when((z < Z - 1) & (z - k >= 0))
            def _():
                sent(hid.at[slices[f]], zr_s.at[k * shares + f])

            @pl.when((z > 0) & (z + k <= Z - 1))
            def _():
                sent(hid.at[slices[f]], zl_s.at[k * shares + f])
    for b in range(S):
        @pl.when(b != s)
        def _():
            for f in range(shares):
                sent(hid.at[slices[f]], pl_s.at[b * shares + f])
            sent(gs.at[b], g_s.at[b])
        for f in range(shares):
            sent(hid.at[slices[f]], mt_s.at[b * shares + f])
        sent(cot, cm_s.at[b])
        sent(px_rx.at[b], px_s.at[b])

        @pl.when((z >= s) & (z < Z - 1))
        def _():
            sent(cot, cr_s.at[b])

        @pl.when((z <= s) & (z > 0))
        def _():
            sent(cot, cl_s.at[b])
    for q in range(Z):
        @pl.when(q != z)
        def _():
            sent(gs.at[0], f_s.at[q])

    @pl.when(s != z)
    def _():
        sent(cot, cp_s)
    for r in range(1, S):
        sent(tid_tx, id_s.at[r - 1])
        sent(info.at[0], in_s.at[r - 1])
    for n in range(6 * steps):
        sent(snd.at[0, low[0]], rs_s.at[n])
        sent(cd.at[0, low[0]], ag_s.at[n])
    for r in range(1, V):
        sent(stat_tx, st_s.at[r - 1])


def put_out(loss, hgrad, tied, loss_out, hgrad_out, tied_out, sems):
    moves = [
        pltpu.make_async_copy(src, dst, sems.at[i])
        for i, (src, dst) in enumerate(((tied, tied_out), (hgrad, hgrad_out), (loss, loss_out)))
    ]
    for move in moves:
        move.start()
    for move in moves:
        move.wait()


def fused(hidden, slab, token_ids, target_ids, input_cot, loss_grad):
    S = lax.axis_size("section")
    V = lax.axis_size("vocab")
    Z = V // 2
    T, W = hidden.shape
    R, Q = slab.shape
    vm = pltpu.VMEM
    dma = pltpu.SemaphoreType.DMA
    half = vm((S, W, T), bf16)
    both = vm((S // 2, Q, 2 * T), bf16)
    scratch = [
        vm((W, T), bf16), vm((W, T), bf16),
        vm((1, T), jnp.int32), vm((1, T), jnp.int32), vm((1, T), f32),
        vm((R, Q), bf16), half, half, half, both,
        vm((S, R, T), jnp.int16), vm((3, R, T), jnp.int16), vm((R, T), f32),
        half, half, both, vm((S, 8, T), jnp.int32), vm((8, T), jnp.int32),
        vm((S, R, T), jnp.int16), vm((16, T), f32), vm((V, 16, T), f32),
        vm((S, 8, T), f32), vm((S, R, T), bf16), vm((S, Q, T), f32), vm((S, W, T), f32), half, half, vm((Z, W, T), bf16),
        dma((6,)), *[dma((Z * shares,))] * 4,
        *[dma((S * shares,))] * 4, dma, dma((S,)),
        dma((S,)), dma((S,)), dma((S,)), dma((S,)), dma((S,)), dma((S,)), dma((S,)),
        dma((S,)), dma((S,)),
        dma((6 * steps,)), dma((6 * steps,)), dma((V,)), dma((V,)), dma((6 * steps,)), dma((6 * steps,)),
        dma((S,)), dma((S,)), dma((S,)), dma((S,)), dma((Z,)), dma((Z,)),
    ]
    block = pl.BlockSpec(memory_space=vm)
    anywhere = pl.BlockSpec(memory_space=pl.ANY)
    far_memory = pl.BlockSpec(memory_space=pltpu.HBM)
    results = pl.pallas_call(
        functools.partial(fused_kernel, (S, V)),
        out_shape=(
            jax.ShapeDtypeStruct((1, T), f32),
            jax.ShapeDtypeStruct((W, T), bf16),
            jax.ShapeDtypeStruct((R, Q), bf16),
        ),
        in_specs=[far_memory] * 6,
        out_specs=(block, block, block),
        scratch_shapes=scratch,
        compiler_params=pltpu.CompilerParams(
            collective_id=0, has_side_effects=True, vmem_limit_bytes=48 * 2**20
        ),
        name="fused",
    )(
        *(
            pltpu.with_memory_space_constraint(x, pltpu.HBM)
            for x in (
                hidden.T, input_cot.T, slab,
                token_ids.reshape(1, T), target_ids.reshape(1, T), loss_grad.reshape(1, T),
            )
        )
    )
    loss, hgrad, tied = pl.pallas_call(
        put_out,
        out_shape=tuple(jax.ShapeDtypeStruct(x.shape, x.dtype) for x in results),
        in_specs=[block] * 3,
        out_specs=(anywhere,) * 3,
        scratch_shapes=[dma((3,))],
        compiler_params=pltpu.CompilerParams(vmem_limit_bytes=8 * 2**20),
        name="put_out",
    )(*results)
    return loss.reshape(T), hgrad.T, tied


def from_partner(block, axis, stride):
    count = lax.axis_size(axis)
    route = []
    for low in range(count):
        high = low | 1 << stride
        if high != low and high < count:
            route += [(low, high), (high, low)]
    return lax.ppermute(block, axis, route)


def left_product(left_side, right_side):
    return lax.dot_general(
        left_side, right_side, (((0,), (0,)), ((), ())), preferred_element_type=jnp.float32
    )


def local_parts(raw_logits, targets, columns):
    capped = logit_cap * jnp.tanh(raw_logits / logit_cap)
    exp_logits = jnp.exp(capped)
    target_hit = (targets[:, None] == columns[None, :]).astype(jnp.float32)
    local_total = jnp.sum(exp_logits, axis=1)
    local_pick = jnp.sum(target_hit * capped, axis=1)
    return (capped, exp_logits, target_hit, local_total, local_pick)


def finish(capped, exp_logits, target_hit, exp_total, picked, scales):
    token_loss = jnp.log(exp_total) - picked
    slope = 1.0 - (capped / logit_cap) ** 2
    dlogit = (scales[:, None] * (exp_logits / exp_total[:, None] - target_hit) * slope).astype(
        jnp.bfloat16
    )
    return (token_loss, dlogit)


def general(hidden, slab, token_ids, target_ids, input_cot, loss_grad):
    rows_here = slab.shape[0]
    quarter_width = slab.shape[1]
    sections = lax.axis_size("section")
    shards = lax.axis_size("vocab")
    model_width = quarter_width * sections
    own_tokens = hidden.shape[0]
    share_width = hidden.shape[1]
    full_hidden, full_cot = (
        lax.all_gather(hidden, "vocab", axis=1, tiled=True),
        lax.all_gather(input_cot, "vocab", axis=1, tiled=True),
    )
    hidden_part, cot_part = (
        lax.all_to_all(full_hidden, "section", split_axis=1, concat_axis=0, tiled=True),
        lax.all_to_all(full_cot, "section", split_axis=1, concat_axis=0, tiled=True),
    )
    partial_value = lax.dot_general(
        hidden_part, slab, (((1,), (1,)), ((), ())), preferred_element_type=jnp.float32
    )
    columns = lax.axis_index("vocab") * rows_here + jnp.arange(rows_here, dtype=jnp.int32)
    raw_logits = lax.psum_scatter(partial_value, "section", scatter_dimension=0, tiled=True)
    capped, exp_logits, target_hit, local_total, local_pick = local_parts(
        raw_logits, target_ids, columns
    )
    exp_total, picked = lax.psum((local_total, local_pick), "vocab")
    token_loss, dlogit = finish(capped, exp_logits, target_hit, exp_total, picked, loss_grad)
    all_ids = lax.all_gather(token_ids, "section", axis=0, tiled=True)
    all_dlogit = lax.all_gather(dlogit, "section", axis=0, tiled=True)
    total_tokens = all_dlogit.shape[0]
    blocks = shards // sections
    narrow = share_width // sections
    arranged_slab = slab.reshape(rows_here, blocks, sections, narrow)
    term = jnp.einsum(
        "tv,vkrw->trkw", all_dlogit, arranged_slab, preferred_element_type=jnp.float32
    )
    term = term.reshape(total_tokens, shards * narrow)
    piece = lax.psum_scatter(term, "vocab", scatter_dimension=1, tiled=True).astype(jnp.bfloat16)
    slots = lax.all_to_all(piece, "section", split_axis=0, concat_axis=0, tiled=True).reshape(
        sections, own_tokens, narrow
    )
    base_bit = blocks.bit_length() - 1
    rank_high = lax.axis_index("vocab") // blocks
    for level in range(sections.bit_length() - 1):
        span = 1 << level
        shaped = slots.reshape(sections // (2 * span), 2, span, own_tokens, narrow)
        mine_bit = rank_high // span % 2
        lower = shaped[:, 0]
        upper = shaped[:, 1]
        keep = jnp.where(mine_bit == 0, lower, upper)
        outgoing = jnp.where(mine_bit == 0, upper, lower)
        incoming = from_partner(outgoing, "vocab", base_bit + level)
        first = jnp.where(mine_bit == 0, keep, incoming)
        second = jnp.where(mine_bit == 0, incoming, keep)
        slots = jnp.stack([first, second], axis=1).reshape(sections, own_tokens, narrow)
    hidden_grad = jnp.transpose(slots, (1, 0, 2)).reshape(own_tokens, sections * narrow)
    onehot = (all_ids[:, None] == columns[None, :]).astype(jnp.bfloat16)
    embed_scale = math.sqrt(model_width)
    tied_grad = left_product(all_dlogit, hidden_part) + left_product(onehot, cot_part) * embed_scale
    return (token_loss, hidden_grad, tied_grad.astype(jnp.bfloat16))


def on_device(hidden, slab, token_ids, target_ids, input_cot, loss_grad):
    sections = lax.axis_size("section")
    shards = lax.axis_size("vocab")
    fits = (
        sections == 4
        and shards == 2 * sections
        and hidden.shape[0] % 128 == 0
        and slab.shape[0] % 2048 == 0
        and hidden.shape[1] % 32 == 0
    )
    step = fused if fits else general
    return step(hidden, slab, token_ids, target_ids, input_cot, loss_grad)


def solution(mesh):
    placed = (
        P("section", "vocab"),
        P("vocab", "section"),
        P("section"),
        P("section"),
        P("section", "vocab"),
        P("section"),
    )
    return jax.shard_map(
        on_device,
        mesh=mesh,
        in_specs=placed,
        out_specs=(P("section"), P("section", "vocab"), P("vocab", "section")),
        check_vma=False,
    )
```

```python
import functools
import math

import jax
import jax.numpy as jnp
from jax import lax
from jax.experimental import pallas as pl
from jax.experimental.pallas import tpu as pltpu
from jax.sharding import PartitionSpec as P

logit_cap = 30.0
code_knee = 16.0
code_top = 32767.0
f32 = jnp.float32
bf16 = jnp.bfloat16


steps = 4
shares = 2


def encode(x):
    y = x / (jnp.abs(x) + code_knee) * code_top
    return jnp.floor(y + 0.5).astype(jnp.int32).astype(jnp.int16)


def decode(code):
    y = code.astype(jnp.int32).astype(f32) * (1.0 / code_top)
    return code_knee * y / (1.0 - jnp.abs(y))


def over_tokens(left, right):
    return lax.dot_general(
        left, right, (((1,), (1,)), ((), ())), preferred_element_type=jnp.float32
    )


def fused_kernel(
    dims, hid_hbm, cot_hbm, slab_hbm, tok_hbm, tgt_hbm, scale_hbm, loss, hgrad, tied,
    hid, cot, tok, tgt, scale,
    slab, zg, hq, hm, h, snd, rcv, own, cq, cm, cf, ids, tid_tx, cd, stat_tx, stat_rx,
    info, dl, gp, gt, px_rx, gs, zr, fin, zf, zsum, whole,
    in_sem, zr_s, zr_r, zl_s, zl_r, pl_s, pl_r, mt_s, mt_r, cp_s, cp_r, cr_s, cl_s, cz_r,
    cm_s, cm_r, id_s, id_r, in_s, in_r, rs_s, rs_r, st_s, st_r, ag_s, ag_r, px_s, px_r, g_s, g_r, f_s, f_r, zf_s, zf_r, zw_s, zw_r,
):
    S, V = dims
    Z = V // 2
    W, T = hid.shape
    R, Q = slab.shape
    span = R // steps
    half = span // 2
    s = lax.axis_index("section")
    v = lax.axis_index("vocab")
    z = v // 2
    c = v % 2
    mate = z * 2 + 1 - c
    nx, ny, far = s ^ 1, s ^ 2, s ^ 3
    tile = 256

    def rc(src, dst, ssem, rsem, dev):
        return pltpu.make_async_remote_copy(
            src_ref=src, dst_ref=dst, send_sem=ssem, recv_sem=rsem,
            device_id=dev, device_id_type=pl.DeviceIdType.MESH,
        )

    def got(ref, rsem):
        rc(ref, ref, rsem, rsem, (s, mate)).wait_recv()

    def sent(ref, ssem):
        rc(ref, ref, ssem, ssem, (s, mate)).wait_send()

    loads = [
        pltpu.make_async_copy(src, dst, in_sem.at[i])
        for i, (src, dst) in enumerate(
            ((hid_hbm, hid), (cot_hbm, cot), (tok_hbm, tok), (tgt_hbm, tgt), (scale_hbm, scale), (slab_hbm, slab))
        )
    ]
    for load in loads:
        load.start()

    bar = pltpu.get_barrier_semaphore()
    for r in range(1, S):
        pl.semaphore_signal(bar, inc=1, device_id=((s + r) % S, v), device_id_type=pl.DeviceIdType.MESH)
    for r in range(1, V):
        pl.semaphore_signal(bar, inc=1, device_id=(s, (v + r) % V), device_id_type=pl.DeviceIdType.MESH)
    for load in loads[:5]:
        load.wait()
    both_ids = jnp.concatenate([jnp.broadcast_to(x[...], (4, T)) for x in (tok, tgt)], axis=0)
    tid_tx[...] = both_ids
    ids[s] = both_ids
    pl.semaphore_wait(bar, S + V - 2)

    piece = W // shares
    slices = [slice(f * piece, (f + 1) * piece) for f in range(shares)]

    def z_send(k, f):
        part = slices[f]
        n = k * shares + f
        b = z - k

        @pl.when((z < Z - 1) & (b >= 0))
        def _():
            src = hid.at[part] if k == 0 else zg.at[b, part]
            rc(src, zg.at[b, part], zr_s.at[n], zr_r.at[n], (s, v + 2)).start()

        d = z + k

        @pl.when((z > 0) & (d <= Z - 1))
        def _():
            src = hid.at[part] if k == 0 else zg.at[d, part]
            rc(src, zg.at[d, part], zl_s.at[n], zl_r.at[n], (s, v - 2)).start()

    def plane_send(b, src, f):
        part = slices[f]

        @pl.when(b != s)
        def _():
            rc(src, hq.at[s, part], pl_s.at[b * shares + f], pl_r.at[s * shares + f], (b, v)).start()

        @pl.when(b == s)
        def _():
            n = s * shares + f
            rc(src, hm.at[s, part], mt_s.at[n], mt_r.at[n], (s, mate)).start()
            hq[s, part] = src[...]

    for f in range(shares):
        z_send(0, f)
    for f in range(shares):
        plane_send(z, hid.at[slices[f]], f)

    @pl.when(s != z)
    def _():
        rc(cot, cq.at[s], cp_s, cp_r.at[s], (z, v)).start()

    for r in range(1, S):
        t = (s + r) % S
        rc(tid_tx, ids.at[s], id_s.at[r - 1], id_r.at[s], (t, v)).start()

    for k in range(Z - 1):
        b = z - 1 - k
        d = z + 1 + k
        for f in range(shares):
            part = slices[f]
            n = k * shares + f

            @pl.when(b >= 0)
            def _():
                got(zg.at[b, part], zr_r.at[n])

            @pl.when(d <= Z - 1)
            def _():
                got(zg.at[d, part], zl_r.at[n])

            if k + 1 < Z - 1:
                z_send(k + 1, f)

            @pl.when(b >= 0)
            def _():
                plane_send(b, zg.at[b, part], f)

            @pl.when(d <= Z - 1)
            def _():
                plane_send(d, zg.at[d, part], f)

    def forward(src, t):
        @pl.when((z >= s) & (z < Z - 1))
        def _():
            rc(src, cq.at[t], cr_s.at[t], cz_r.at[t], (s, v + 2)).start()

        @pl.when((z <= s) & (z > 0))
        def _():
            rc(src, cq.at[t], cl_s.at[t], cz_r.at[t], (s, v - 2)).start()

        rc(src, cm.at[t], cm_s.at[t], cm_r.at[t], (s, mate)).start()

    @pl.when(z == s)
    def _():
        cq[s] = cot[...]
        forward(cot, s)
        for r in range(1, S):
            t = (s + r) % S
            got(cq.at[t], cp_r.at[t])
            forward(cq.at[t], t)

    apart = jnp.abs(z - s)

    def pass_cot(distance, first, last):
        @pl.when(apart == distance)
        def _():
            for r in range(first, last):
                t = (s + r) % S
                got(cq.at[t], cz_r.at[t])
                forward(cq.at[t], t)

    for f in range(shares):
        for r in range(1, S):
            t = s ^ r
            n = t * shares + f
            got(hq.at[t, slices[f]], pl_r.at[n])
            rc(hq.at[t, slices[f]], hm.at[t, slices[f]], mt_s.at[n], mt_r.at[n], (s, mate)).start()

    def assemble(full, mine, other, t):
        cols = slice(t % 2 * T, (t % 2 + 1) * T)
        full[t // 2, pl.ds(pl.multiple_of(c * W, 16), W), cols] = mine[t]
        full[t // 2, pl.ds(pl.multiple_of((1 - c) * W, 16), W), cols] = other[t]

    for t in range(S):
        for f in range(shares):
            got(hm.at[t, slices[f]], mt_r.at[t * shares + f])
        assemble(h, hq, hm, t)
    loads[5].wait()

    low = [slice(k * span, k * span + half) for k in range(steps)]
    high = [slice(k * span + half, (k + 1) * span) for k in range(steps)]
    other = 1 - s // 2
    even = s % 2 == 0

    def logits(k):
        def logit_tile(j, carry):
            rows = pl.ds(pl.multiple_of(k * span + j * tile, tile), tile)
            part = jnp.dot(slab[rows, :], h[other], preferred_element_type=f32)
            for m in range(2):
                snd[2 * other + m, rows, :] = encode(part[:, m * T:(m + 1) * T])
            part = jnp.dot(slab[rows, :], h[s // 2], preferred_element_type=f32)
            own[rows, :] = jnp.where(even, part[:, :T], part[:, T:])
            snd[nx, rows, :] = encode(jnp.where(even, part[:, T:], part[:, :T]))
            return carry

        lax.fori_loop(0, span // tile, logit_tile, 0)

    def logit_send(n, t, slot, part, to):
        rc(snd.at[t, part], rcv.at[slot, part], rs_s.at[n], rs_r.at[n], (to, v)).start()

    def logit_got(n, slot, part):
        got(rcv.at[slot, part], rs_r.at[n])

    def relay(t, part):
        def relay_tile(j, carry):
            rows = pl.ds(pl.multiple_of(part.start + j * tile, tile), tile)
            snd[t, rows, :] = encode(decode(snd[t, rows, :]) + decode(rcv[2, rows, :]))
            return carry

        lax.fori_loop(0, half // tile, relay_tile, 0)

    def logit_start(k):
        logit_send(6 * k, far, 2, low[k], nx)
        logit_send(6 * k + 1, far, 2, high[k], ny)
        logit_send(6 * k + 2, nx, 0, low[k], nx)
        logit_send(6 * k + 3, ny, 1, high[k], ny)

    def logit_relay(k):
        logit_got(6 * k, 2, low[k])
        relay(ny, low[k])
        logit_send(6 * k + 4, ny, 1, low[k], ny)
        logit_got(6 * k + 1, 2, high[k])
        relay(nx, high[k])
        logit_send(6 * k + 5, nx, 0, high[k], nx)

    soft = 128
    target = tgt[...]
    unit = logit_cap / code_top

    def row_ids(j, n, width):
        return v * R + j * n + lax.broadcasted_iota(jnp.int32, (n, width), 0)

    def softmax_sums(k, sums):
        logit_got(6 * k + 2, 0, low[k])
        logit_got(6 * k + 3, 1, high[k])
        logit_got(6 * k + 4, 1, low[k])
        logit_got(6 * k + 5, 0, high[k])

        def soft_tile(j, carry):
            total, pick = carry
            rows = pl.ds(pl.multiple_of(j * soft, soft), soft)
            raw = own[rows, :] + decode(rcv[0, rows, :]) + decode(rcv[1, rows, :])
            bent = jnp.tanh(raw / logit_cap)
            code = jnp.floor(bent * code_top + 0.5)
            cd[s, rows, :] = code.astype(jnp.int32).astype(jnp.int16)
            hit = row_ids(j, soft, T) == target
            total = total + jnp.sum(jnp.exp(code * unit), axis=0, keepdims=True)
            pick = pick + jnp.sum(jnp.where(hit, logit_cap * bent, 0.0), axis=0, keepdims=True)
            return total, pick

        count = span // soft
        return lax.fori_loop(k * count, (k + 1) * count, soft_tile, sums)

    def code_send(n, t, part, to):
        block = cd.at[t, part]
        rc(block, block, ag_s.at[n], ag_r.at[n], (to, v)).start()

    def code_got(n, t, part):
        got(cd.at[t, part], ag_r.at[n])

    def code_start(k):
        code_send(6 * k, s, high[k], nx)
        code_send(6 * k + 1, s, low[k], ny)
        code_send(6 * k + 2, s, low[k], nx)
        code_send(6 * k + 3, s, high[k], ny)

    def code_relay(k):
        code_got(6 * k + 1, ny, low[k])
        code_send(6 * k + 4, ny, low[k], nx)
        code_got(6 * k, nx, high[k])
        code_send(6 * k + 5, nx, high[k], ny)

    def info_got(t):
        got(info.at[t], in_r.at[t])

    def grad(t, k):
        scale_row = info[t][0:1, :]
        gain_row = info[t][1:2, :]
        target_row = ids[t][4:5, :]

        def grad_tile(j, carry):
            rows = pl.ds(pl.multiple_of(j * soft, soft), soft)
            code = cd[t, rows, :].astype(jnp.int32).astype(f32)
            hit = row_ids(j, soft, T) == target_row
            slope = 1.0 - (code * (1.0 / code_top)) ** 2
            away = jnp.exp(code * unit) * scale_row - jnp.where(hit, gain_row, 0.0)
            dl[t, rows, :] = (away * slope).astype(bf16)
            return carry

        count = span // soft
        lax.fori_loop(k * count, (k + 1) * count, grad_tile, 0)

    zero = jnp.zeros((1, T), f32)
    sums = (zero, zero)
    for k in range(steps):
        logits(k)
        logit_start(k)
        if k:
            logit_relay(k - 1)
    pass_cot(1, 0, 2)
    sums = softmax_sums(0, sums)
    for k in range(1, steps - 2):
        sums = softmax_sums(k, sums)
    logit_relay(steps - 1)
    pass_cot(1, 2, S)
    for k in range(steps - 2):
        code_start(k)
    pass_cot(2, 0, 2)
    sums = softmax_sums(steps - 2, sums)
    code_start(steps - 2)
    total, pick = softmax_sums(steps - 1, sums)
    stat_tx[0:8, :] = jnp.broadcast_to(total, (8, T))
    stat_tx[8:16, :] = jnp.broadcast_to(pick, (8, T))
    for r in range(1, V):
        rc(stat_tx, stat_rx.at[v], st_s.at[r - 1], st_r.at[v], (s, (v + r) % V)).start()
    stat_rx[v] = stat_tx[...]
    for r in range(1, S):
        t = (s + r) % S
        got(ids.at[t], id_r.at[t])
    code_relay(0)
    pass_cot(2, 2, S)
    for r in range(1, V):
        u = (v + r) % V
        got(stat_rx.at[u], st_r.at[u])
    sums = stat_rx[0]
    for u in range(1, V):
        sums = sums + stat_rx[u]
    total = sums[0:1, :]
    loss[...] = jnp.log(total) - sums[8:9, :]
    gain = scale[...]
    info[s] = jnp.concatenate(
        [gain / total, jnp.broadcast_to(gain, (7, T))], axis=0
    )
    for r in range(1, S):
        t = s ^ r
        rc(info.at[s], info.at[s], in_s.at[r - 1], in_r.at[s], (t, v)).start()
    code_start(steps - 1)

    def rows_term(t, part):
        return lax.dot_general(
            dl[t, part], slab[part], (((0,), (0,)), ((), ())), preferred_element_type=f32
        )

    def give(t, g):
        gt[t] = g.T
        block = gt.at[t, pl.ds(pl.multiple_of((1 - c) * W, 16), W)]
        rc(block, px_rx.at[t], px_s.at[t], px_r.at[t], (s, mate)).start()

    def term(t):
        give(t, rows_term(t, slice(0, R)))

    lead, rest = slice(0, W // 2), slice(W // 2, W)

    def fin_send(q, src, part):
        @pl.when(q != z)
        def _():
            rc(src, fin.at[z, part], f_s.at[q], f_r.at[z], (s, 2 * q + c)).start()

        @pl.when(q == z)
        def _():
            fin[z, part] = src[...]

    def pass_on(t):
        got(px_rx.at[t], px_r.at[t])
        kept = gt[t, pl.ds(pl.multiple_of(c * W, 16), W), :]
        gs[t] = (kept + px_rx[t]).astype(bf16)

    def pass_near(t):
        pass_on(t)
        rc(gs.at[t], zr.at[s], g_s.at[t], g_r.at[s], (t, v)).start()

    def pass_far():
        pass_on(far)

        @pl.when(z != s)
        def _():
            rc(gs.at[far, rest], zf.at[z], zf_s, zf_r.at[z], (s, 2 * s + c)).start()

        @pl.when(z == s)
        def _():
            zf[z] = gs[far, rest]

        rc(gs.at[far, lead], zr.at[s, lead], g_s.at[far], g_r.at[s], (far, v)).start()

    def gather_far():
        @pl.when(z == s)
        def _():
            for r in range(1, Z):
                u = (z + r) % Z
                got(zf.at[u], zf_r.at[u])
            acc = zf[0].astype(f32)
            for u in range(1, Z):
                acc = acc + zf[u].astype(f32)
            zsum[...] = acc.astype(bf16)
            rc(zsum, whole, zw_s, zw_r, (far, v)).start()

    for k in range(steps):
        grad(s, k)
    term(s)
    code_relay(1)
    for t in (nx, ny):
        info_got(t)

    def near_got(k):
        code_got(6 * k + 2, nx, low[k])
        code_got(6 * k + 3, ny, high[k])
        grad(nx, k)
        grad(ny, k)

    def far_got(k):
        code_got(6 * k + 4, far, low[k])
        code_got(6 * k + 5, far, high[k])
        grad(far, k)

    near_got(0)
    pass_on(s)
    fin_send(s, gs.at[s], slice(0, W))
    near_got(1)
    code_relay(2)
    near_got(2)
    info_got(far)
    far_got(0)
    code_relay(3)
    code_got(20, nx, low[3])
    grad(nx, 3)
    term(nx)
    code_got(21, ny, high[3])
    grad(ny, 3)
    term(ny)
    far_got(1)
    far_got(2)
    pass_near(nx)
    early = slice(0, (steps - 1) * span)
    gp[...] = rows_term(far, early)
    pass_near(ny)
    far_got(3)
    give(far, gp[...] + rows_term(far, slice(early.stop, R)))

    def drain():
        for k in range(Z - 1):
            for f in range(shares):
                @pl.when((z < Z - 1) & (z - k >= 0))
                def _():
                    sent(hid.at[slices[f]], zr_s.at[k * shares + f])

                @pl.when((z > 0) & (z + k <= Z - 1))
                def _():
                    sent(hid.at[slices[f]], zl_s.at[k * shares + f])
        for b in range(S):
            @pl.when(b != s)
            def _():
                for f in range(shares):
                    sent(hid.at[slices[f]], pl_s.at[b * shares + f])
            for f in range(shares):
                sent(hid.at[slices[f]], mt_s.at[b * shares + f])
            sent(cot, cm_s.at[b])
            sent(px_rx.at[b], px_s.at[b])

            @pl.when((z >= s) & (z < Z - 1))
            def _():
                sent(cot, cr_s.at[b])

            @pl.when((z <= s) & (z > 0))
            def _():
                sent(cot, cl_s.at[b])

        @pl.when(s != z)
        def _():
            sent(cot, cp_s)
        for r in range(1, S):
            sent(tid_tx, id_s.at[r - 1])
            sent(info.at[0], in_s.at[r - 1])
        for n in range(6 * steps):
            sent(snd.at[0, low[0]], rs_s.at[n])
            sent(cd.at[0, low[0]], ag_s.at[n])
        for r in range(1, V):
            sent(stat_tx, st_s.at[r - 1])

    def fin_pass(q, part):
        got(zr.at[q, part], g_r.at[q])
        fin_send(q, zr.at[q, part], part)

    every = jnp.concatenate([ids[t][0:1, :] for t in range(S)], axis=1)
    root = math.sqrt(Q * S)

    def tied_tile(j, carry):
        rows = pl.ds(pl.multiple_of(j * tile, tile), tile)
        onehot = (row_ids(j, tile, S * T) == every).astype(f32).astype(bf16)
        head, embed = 0.0, 0.0
        for p in range(S // 2):
            lhs = jnp.concatenate([dl[2 * p, rows, :], dl[2 * p + 1, rows, :]], axis=1)
            head = head + over_tokens(lhs, h[p])
            embed = embed + over_tokens(onehot[:, 2 * p * T:2 * (p + 1) * T], cf[p])
        tied[rows, :] = (head + embed * root).astype(bf16)
        return carry

    tiles = R // tile
    marks = [0, tiles // 8, tiles // 2, tiles]
    pass_far()
    for distance in range(3, Z):
        pass_cot(distance, 0, S)
    for t in range(S):
        got(cm.at[t], cm_r.at[t])
        assemble(cf, cq, cm, t)
    lax.fori_loop(marks[0], marks[1], tied_tile, 0)
    drain()
    fin_pass(nx, slice(0, W))
    fin_pass(ny, slice(0, W))
    fin_pass(far, lead)
    lax.fori_loop(marks[1], marks[2], tied_tile, 0)
    gather_far()
    lax.fori_loop(marks[2], marks[3], tied_tile, 0)

    def fin_sum(part):
        for r in range(1, Z):
            u = (z + r) % Z
            got(fin.at[u, part], f_r.at[u])
        acc = fin[0, part].astype(f32)
        for u in range(1, Z):
            acc = acc + fin[u, part].astype(f32)
        hgrad[part] = acc.astype(bf16)

    @pl.when(z == far)
    def _():
        fin_sum(lead)
        got(whole, zw_r)
        hgrad[rest] = whole[...]

    @pl.when(z != far)
    def _():
        fin_sum(slice(0, W))


    for r in range(1, S):
        part = lead if r == 3 else slice(0, W)
        sent(gs.at[0, part], g_s.at[s ^ r])
    for r in range(S):
        part = lead if r == 3 else slice(0, W)

        @pl.when(s ^ r != z)
        def _():
            sent(gs.at[0, part], f_s.at[s ^ r])

    @pl.when(z != s)
    def _():
        sent(gs.at[0, rest], zf_s)

    @pl.when(z == s)
    def _():
        sent(zsum, zw_s)


def put_out(loss, hgrad, tied, loss_out, hgrad_out, tied_out, sems):
    count = sems.shape[0] - 2
    rows = tied.shape[0] // count
    pairs = [(tied.at[pl.ds(n * rows, rows)], tied_out.at[pl.ds(n * rows, rows)]) for n in range(count)]
    pairs += [(hgrad, hgrad_out), (loss, loss_out)]
    moves = [pltpu.make_async_copy(src, dst, sems.at[i]) for i, (src, dst) in enumerate(pairs)]
    for move in moves:
        move.start()
    for move in moves:
        move.wait()


def fused(hidden, slab, token_ids, target_ids, input_cot, loss_grad):
    S = lax.axis_size("section")
    V = lax.axis_size("vocab")
    Z = V // 2
    T, W = hidden.shape
    R, Q = slab.shape
    vm = pltpu.VMEM
    dma = pltpu.SemaphoreType.DMA
    half = vm((S, W, T), bf16)
    both = vm((S // 2, Q, 2 * T), bf16)
    scratch = [
        vm((W, T), bf16), vm((W, T), bf16),
        vm((1, T), jnp.int32), vm((1, T), jnp.int32), vm((1, T), f32),
        vm((R, Q), bf16), half, half, half, both,
        vm((S, R, T), jnp.int16), vm((3, R, T), jnp.int16), vm((R, T), f32),
        half, half, both, vm((S, 8, T), jnp.int32), vm((8, T), jnp.int32),
        vm((S, R, T), jnp.int16), vm((16, T), f32), vm((V, 16, T), f32),
        vm((S, 8, T), f32), vm((S, R, T), bf16), vm((T, Q), f32), vm((S, Q, T), f32), vm((S, W, T), f32), half, half, vm((Z, W, T), bf16),
        vm((Z, W // 2, T), bf16), vm((W // 2, T), bf16), vm((W // 2, T), bf16),
        dma((6,)), *[dma((Z * shares,))] * 4,
        *[dma((S * shares,))] * 4, dma, dma((S,)),
        dma((S,)), dma((S,)), dma((S,)), dma((S,)), dma((S,)), dma((S,)), dma((S,)),
        dma((S,)), dma((S,)),
        dma((6 * steps,)), dma((6 * steps,)), dma((V,)), dma((V,)), dma((6 * steps,)), dma((6 * steps,)),
        dma((S,)), dma((S,)), dma((S,)), dma((S,)), dma((Z,)), dma((Z,)),
        dma, dma((Z,)), dma, dma,
    ]
    block = pl.BlockSpec(memory_space=vm)
    anywhere = pl.BlockSpec(memory_space=pl.ANY)
    far_memory = pl.BlockSpec(memory_space=pltpu.HBM)
    results = pl.pallas_call(
        functools.partial(fused_kernel, (S, V)),
        out_shape=(
            jax.ShapeDtypeStruct((1, T), f32),
            jax.ShapeDtypeStruct((W, T), bf16),
            jax.ShapeDtypeStruct((R, Q), bf16),
        ),
        in_specs=[far_memory] * 6,
        out_specs=(block, block, block),
        scratch_shapes=scratch,
        compiler_params=pltpu.CompilerParams(
            collective_id=0, has_side_effects=True, vmem_limit_bytes=48 * 2**20
        ),
        name="fused",
    )(
        *(
            pltpu.with_memory_space_constraint(x, pltpu.HBM)
            for x in (
                hidden.T, input_cot.T, slab,
                token_ids.reshape(1, T), target_ids.reshape(1, T), loss_grad.reshape(1, T),
            )
        )
    )
    loss, hgrad, tied = pl.pallas_call(
        put_out,
        out_shape=tuple(jax.ShapeDtypeStruct(x.shape, x.dtype) for x in results),
        in_specs=[block] * 3,
        out_specs=(anywhere,) * 3,
        scratch_shapes=[dma((10,))],
        compiler_params=pltpu.CompilerParams(vmem_limit_bytes=8 * 2**20),
        name="put_out",
    )(*results)
    return loss.reshape(T), hgrad.T, tied


def from_partner(block, axis, stride):
    count = lax.axis_size(axis)
    route = []
    for low in range(count):
        high = low | 1 << stride
        if high != low and high < count:
            route += [(low, high), (high, low)]
    return lax.ppermute(block, axis, route)


def left_product(left_side, right_side):
    return lax.dot_general(
        left_side, right_side, (((0,), (0,)), ((), ())), preferred_element_type=jnp.float32
    )


def local_parts(raw_logits, targets, columns):
    capped = logit_cap * jnp.tanh(raw_logits / logit_cap)
    exp_logits = jnp.exp(capped)
    target_hit = (targets[:, None] == columns[None, :]).astype(jnp.float32)
    local_total = jnp.sum(exp_logits, axis=1)
    local_pick = jnp.sum(target_hit * capped, axis=1)
    return (capped, exp_logits, target_hit, local_total, local_pick)


def finish(capped, exp_logits, target_hit, exp_total, picked, scales):
    token_loss = jnp.log(exp_total) - picked
    slope = 1.0 - (capped / logit_cap) ** 2
    dlogit = (scales[:, None] * (exp_logits / exp_total[:, None] - target_hit) * slope).astype(
        jnp.bfloat16
    )
    return (token_loss, dlogit)


def general(hidden, slab, token_ids, target_ids, input_cot, loss_grad):
    rows_here = slab.shape[0]
    quarter_width = slab.shape[1]
    sections = lax.axis_size("section")
    shards = lax.axis_size("vocab")
    model_width = quarter_width * sections
    own_tokens = hidden.shape[0]
    share_width = hidden.shape[1]
    full_hidden, full_cot = (
        lax.all_gather(hidden, "vocab", axis=1, tiled=True),
        lax.all_gather(input_cot, "vocab", axis=1, tiled=True),
    )
    hidden_part, cot_part = (
        lax.all_to_all(full_hidden, "section", split_axis=1, concat_axis=0, tiled=True),
        lax.all_to_all(full_cot, "section", split_axis=1, concat_axis=0, tiled=True),
    )
    partial_value = lax.dot_general(
        hidden_part, slab, (((1,), (1,)), ((), ())), preferred_element_type=jnp.float32
    )
    columns = lax.axis_index("vocab") * rows_here + jnp.arange(rows_here, dtype=jnp.int32)
    raw_logits = lax.psum_scatter(partial_value, "section", scatter_dimension=0, tiled=True)
    capped, exp_logits, target_hit, local_total, local_pick = local_parts(
        raw_logits, target_ids, columns
    )
    exp_total, picked = lax.psum((local_total, local_pick), "vocab")
    token_loss, dlogit = finish(capped, exp_logits, target_hit, exp_total, picked, loss_grad)
    all_ids = lax.all_gather(token_ids, "section", axis=0, tiled=True)
    all_dlogit = lax.all_gather(dlogit, "section", axis=0, tiled=True)
    total_tokens = all_dlogit.shape[0]
    blocks = shards // sections
    narrow = share_width // sections
    arranged_slab = slab.reshape(rows_here, blocks, sections, narrow)
    term = jnp.einsum(
        "tv,vkrw->trkw", all_dlogit, arranged_slab, preferred_element_type=jnp.float32
    )
    term = term.reshape(total_tokens, shards * narrow)
    piece = lax.psum_scatter(term, "vocab", scatter_dimension=1, tiled=True).astype(jnp.bfloat16)
    slots = lax.all_to_all(piece, "section", split_axis=0, concat_axis=0, tiled=True).reshape(
        sections, own_tokens, narrow
    )
    base_bit = blocks.bit_length() - 1
    rank_high = lax.axis_index("vocab") // blocks
    for level in range(sections.bit_length() - 1):
        span = 1 << level
        shaped = slots.reshape(sections // (2 * span), 2, span, own_tokens, narrow)
        mine_bit = rank_high // span % 2
        lower = shaped[:, 0]
        upper = shaped[:, 1]
        keep = jnp.where(mine_bit == 0, lower, upper)
        outgoing = jnp.where(mine_bit == 0, upper, lower)
        incoming = from_partner(outgoing, "vocab", base_bit + level)
        first = jnp.where(mine_bit == 0, keep, incoming)
        second = jnp.where(mine_bit == 0, incoming, keep)
        slots = jnp.stack([first, second], axis=1).reshape(sections, own_tokens, narrow)
    hidden_grad = jnp.transpose(slots, (1, 0, 2)).reshape(own_tokens, sections * narrow)
    onehot = (all_ids[:, None] == columns[None, :]).astype(jnp.bfloat16)
    embed_scale = math.sqrt(model_width)
    tied_grad = left_product(all_dlogit, hidden_part) + left_product(onehot, cot_part) * embed_scale
    return (token_loss, hidden_grad, tied_grad.astype(jnp.bfloat16))


def on_device(hidden, slab, token_ids, target_ids, input_cot, loss_grad):
    sections = lax.axis_size("section")
    shards = lax.axis_size("vocab")
    fits = (
        sections == 4
        and shards == 2 * sections
        and hidden.shape[0] % 128 == 0
        and slab.shape[0] % 2048 == 0
        and hidden.shape[1] % 32 == 0
    )
    step = fused if fits else general
    return step(hidden, slab, token_ids, target_ids, input_cot, loss_grad)


def solution(mesh):
    placed = (
        P("section", "vocab"),
        P("vocab", "section"),
        P("section"),
        P("section"),
        P("section", "vocab"),
        P("section"),
    )
    return jax.shard_map(
        on_device,
        mesh=mesh,
        in_specs=placed,
        out_specs=(P("section"), P("section", "vocab"), P("vocab", "section")),
        check_vma=False,
    )
```

```python
import functools
import math

import jax
import jax.numpy as jnp
from jax import lax
from jax.experimental import pallas as pl
from jax.experimental.pallas import tpu as pltpu
from jax.sharding import PartitionSpec as P

logit_cap = 30.0
code_knee = 16.0
code_top = 32767.0
f32 = jnp.float32
bf16 = jnp.bfloat16


steps = 4
shares = 2


def encode(x):
    y = x / (jnp.abs(x) + code_knee) * code_top
    return jnp.floor(y + 0.5).astype(jnp.int32).astype(jnp.int16)


def decode(code):
    y = code.astype(jnp.int32).astype(f32) * (1.0 / code_top)
    return code_knee * y / (1.0 - jnp.abs(y))


def over_tokens(left, right):
    return lax.dot_general(
        left, right, (((1,), (1,)), ((), ())), preferred_element_type=jnp.float32
    )


def fused_kernel(
    dims, hid_hbm, cot_hbm, slab_hbm, tok_hbm, tgt_hbm, scale_hbm, loss, hgrad, tied,
    hid, cot, tok, tgt, scale,
    slab, zg, hq, hm, h, snd, rcv, own, cq, cm, cf, ids, tid_tx, cd, stat_tx, stat_rx,
    info, dl, gp, gt, px_rx, gs, zr, fin, zf, zsum, whole, emb,
    in_sem, zr_s, zr_r, zl_s, zl_r, pl_s, pl_r, mt_s, mt_r, cp_s, cp_r, cr_s, cl_s, cz_r,
    cm_s, cm_r, id_s, id_r, in_s, in_r, rs_s, rs_r, st_s, st_r, ag_s, ag_r, px_s, px_r, g_s, g_r, f_s, f_r, zf_s, zf_r, zw_s, zw_r,
):
    S, V = dims
    Z = V // 2
    W, T = hid.shape
    R, Q = slab.shape
    span = R // steps
    half = span // 2
    s = lax.axis_index("section")
    v = lax.axis_index("vocab")
    z = v // 2
    c = v % 2
    mate = z * 2 + 1 - c
    nx, ny, far = s ^ 1, s ^ 2, s ^ 3
    tile = 256

    def rc(src, dst, ssem, rsem, dev):
        return pltpu.make_async_remote_copy(
            src_ref=src, dst_ref=dst, send_sem=ssem, recv_sem=rsem,
            device_id=dev, device_id_type=pl.DeviceIdType.MESH,
        )

    def got(ref, rsem):
        rc(ref, ref, rsem, rsem, (s, mate)).wait_recv()

    def sent(ref, ssem):
        rc(ref, ref, ssem, ssem, (s, mate)).wait_send()

    loads = [
        pltpu.make_async_copy(src, dst, in_sem.at[i])
        for i, (src, dst) in enumerate(
            ((hid_hbm, hid), (cot_hbm, cot), (tok_hbm, tok), (tgt_hbm, tgt), (scale_hbm, scale), (slab_hbm, slab))
        )
    ]
    for load in loads:
        load.start()

    bar = pltpu.get_barrier_semaphore()
    for r in range(1, S):
        pl.semaphore_signal(bar, inc=1, device_id=((s + r) % S, v), device_id_type=pl.DeviceIdType.MESH)
    for r in range(1, V):
        pl.semaphore_signal(bar, inc=1, device_id=(s, (v + r) % V), device_id_type=pl.DeviceIdType.MESH)
    for load in loads[:5]:
        load.wait()
    both_ids = jnp.concatenate([jnp.broadcast_to(x[...], (4, T)) for x in (tok, tgt)], axis=0)
    tid_tx[...] = both_ids
    ids[s] = both_ids
    pl.semaphore_wait(bar, S + V - 2)

    piece = W // shares
    slices = [slice(f * piece, (f + 1) * piece) for f in range(shares)]

    def z_send(k, f):
        part = slices[f]
        n = k * shares + f
        b = z - k

        @pl.when((z < Z - 1) & (b >= 0))
        def _():
            src = hid.at[part] if k == 0 else zg.at[b, part]
            rc(src, zg.at[b, part], zr_s.at[n], zr_r.at[n], (s, v + 2)).start()

        d = z + k

        @pl.when((z > 0) & (d <= Z - 1))
        def _():
            src = hid.at[part] if k == 0 else zg.at[d, part]
            rc(src, zg.at[d, part], zl_s.at[n], zl_r.at[n], (s, v - 2)).start()

    def plane_send(b, src, f):
        part = slices[f]

        @pl.when(b != s)
        def _():
            rc(src, hq.at[s, part], pl_s, pl_r.at[s * shares + f], (b, v)).start()

        @pl.when(b == s)
        def _():
            n = s * shares + f
            rc(src, hm.at[s, part], mt_s, mt_r.at[n], (s, mate)).start()
            hq[s, part] = src[...]

    for f in range(shares):
        z_send(0, f)
    for f in range(shares):
        plane_send(z, hid.at[slices[f]], f)

    @pl.when(s != z)
    def _():
        rc(cot, cq.at[s], cp_s, cp_r.at[s], (z, v)).start()

    for r in range(1, S):
        t = (s + r) % S
        rc(tid_tx, ids.at[s], id_s, id_r.at[s], (t, v)).start()

    for k in range(Z - 1):
        b = z - 1 - k
        d = z + 1 + k
        for f in range(shares):
            part = slices[f]
            n = k * shares + f

            @pl.when(b >= 0)
            def _():
                got(zg.at[b, part], zr_r.at[n])

            @pl.when(d <= Z - 1)
            def _():
                got(zg.at[d, part], zl_r.at[n])

            if k + 1 < Z - 1:
                z_send(k + 1, f)

            @pl.when(b >= 0)
            def _():
                plane_send(b, zg.at[b, part], f)

            @pl.when(d <= Z - 1)
            def _():
                plane_send(d, zg.at[d, part], f)

    def forward(src, t):
        @pl.when((z >= s) & (z < Z - 1))
        def _():
            rc(src, cq.at[t], cr_s.at[t], cz_r.at[t], (s, v + 2)).start()

        @pl.when((z <= s) & (z > 0))
        def _():
            rc(src, cq.at[t], cl_s.at[t], cz_r.at[t], (s, v - 2)).start()

        rc(src, cm.at[t], cm_s, cm_r.at[t], (s, mate)).start()

    @pl.when(z == s)
    def _():
        cq[s] = cot[...]
        forward(cot, s)
        for r in range(1, S):
            t = (s + r) % S
            got(cq.at[t], cp_r.at[t])
            forward(cq.at[t], t)

    apart = jnp.abs(z - s)

    def pass_cot(distance, first, last):
        @pl.when(apart == distance)
        def _():
            for r in range(first, last):
                t = (s + r) % S
                got(cq.at[t], cz_r.at[t])
                forward(cq.at[t], t)

    for f in range(shares):
        for r in range(1, S):
            t = s ^ r
            n = t * shares + f
            got(hq.at[t, slices[f]], pl_r.at[n])
            rc(hq.at[t, slices[f]], hm.at[t, slices[f]], mt_s, mt_r.at[n], (s, mate)).start()

    def assemble(full, mine, other, t):
        cols = slice(t % 2 * T, (t % 2 + 1) * T)
        full[t // 2, pl.ds(pl.multiple_of(c * W, 16), W), cols] = mine[t]
        full[t // 2, pl.ds(pl.multiple_of((1 - c) * W, 16), W), cols] = other[t]

    for t in range(S):
        for f in range(shares):
            got(hm.at[t, slices[f]], mt_r.at[t * shares + f])
        assemble(h, hq, hm, t)
    loads[5].wait()

    low = [slice(k * span, k * span + half) for k in range(steps)]
    high = [slice(k * span + half, (k + 1) * span) for k in range(steps)]
    other = 1 - s // 2
    even = s % 2 == 0

    def logits(k):
        def logit_tile(j, carry):
            rows = pl.ds(pl.multiple_of(k * span + j * tile, tile), tile)
            part = jnp.dot(slab[rows, :], h[other], preferred_element_type=f32)
            for m in range(2):
                snd[2 * other + m, rows, :] = encode(part[:, m * T:(m + 1) * T])
            part = jnp.dot(slab[rows, :], h[s // 2], preferred_element_type=f32)
            own[rows, :] = jnp.where(even, part[:, :T], part[:, T:])
            snd[nx, rows, :] = encode(jnp.where(even, part[:, T:], part[:, :T]))
            return carry

        lax.fori_loop(0, span // tile, logit_tile, 0)

    def logit_send(n, t, slot, part, to):
        rc(snd.at[t, part], rcv.at[slot, part], rs_s, rs_r.at[n], (to, v)).start()

    def logit_got(n, slot, part):
        got(rcv.at[slot, part], rs_r.at[n])

    def relay(t, part):
        def relay_tile(j, carry):
            rows = pl.ds(pl.multiple_of(part.start + j * tile, tile), tile)
            snd[t, rows, :] = encode(decode(snd[t, rows, :]) + decode(rcv[2, rows, :]))
            return carry

        lax.fori_loop(0, half // tile, relay_tile, 0)

    def logit_start(k):
        logit_send(3 * k, far, 2, low[k], nx)
        logit_send(3 * k + 1, far, 2, high[k], ny)
        logit_send(3 * k + 2, nx, 0, low[k], nx)
        logit_send(3 * k + 2, ny, 1, high[k], ny)

    def logit_relay(k):
        logit_got(3 * k, 2, low[k])
        relay(ny, low[k])
        logit_send(3 * k + 2, ny, 1, low[k], ny)
        logit_got(3 * k + 1, 2, high[k])
        relay(nx, high[k])
        logit_send(3 * k + 2, nx, 0, high[k], nx)

    soft = 128
    target = tgt[...]
    unit = logit_cap / code_top

    def row_ids(j, n, width):
        return v * R + j * n + lax.broadcasted_iota(jnp.int32, (n, width), 0)

    def softmax_sums(k, sums):
        logit_got(3 * k + 2, slice(0, 2), slice(k * span, (k + 1) * span))

        def soft_tile(j, carry):
            total, pick = carry
            rows = pl.ds(pl.multiple_of(j * soft, soft), soft)
            raw = own[rows, :] + decode(rcv[0, rows, :]) + decode(rcv[1, rows, :])
            bent = jnp.tanh(raw / logit_cap)
            code = jnp.floor(bent * code_top + 0.5)
            cd[s, rows, :] = code.astype(jnp.int32).astype(jnp.int16)
            hit = row_ids(j, soft, T) == target
            total = total + jnp.sum(jnp.exp(code * unit), axis=0, keepdims=True)
            pick = pick + jnp.sum(jnp.where(hit, logit_cap * bent, 0.0), axis=0, keepdims=True)
            return total, pick

        count = span // soft
        return lax.fori_loop(k * count, (k + 1) * count, soft_tile, sums)

    def code_send(n, t, part, to):
        block = cd.at[t, part]
        rc(block, block, ag_s, ag_r.at[n], (to, v)).start()

    def code_got(n, t, part):
        got(cd.at[t, part], ag_r.at[n])

    def code_start(k):
        code_send(5 * k, s, high[k], nx)
        code_send(5 * k + 1, s, low[k], ny)
        code_send(5 * k + 2, s, low[k], nx)
        code_send(5 * k + 3, s, high[k], ny)

    def code_relay(k):
        code_got(5 * k + 1, ny, low[k])
        code_send(5 * k + 4, ny, low[k], nx)
        code_got(5 * k, nx, high[k])
        code_send(5 * k + 4, nx, high[k], ny)

    def info_got(t):
        got(info.at[t], in_r.at[t])

    def grad(t, k):
        scale_row = info[t][0:1, :]
        gain_row = info[t][1:2, :]
        target_row = ids[t][4:5, :]

        def grad_tile(j, carry):
            rows = pl.ds(pl.multiple_of(j * soft, soft), soft)
            code = cd[t, rows, :].astype(jnp.int32).astype(f32)
            hit = row_ids(j, soft, T) == target_row
            slope = 1.0 - (code * (1.0 / code_top)) ** 2
            away = jnp.exp(code * unit) * scale_row - jnp.where(hit, gain_row, 0.0)
            dl[t, rows, :] = (away * slope).astype(bf16)
            return carry

        count = span // soft
        lax.fori_loop(k * count, (k + 1) * count, grad_tile, 0)

    root = math.sqrt(Q * S)

    def embed_tile(j, carry):
        rows = pl.ds(pl.multiple_of(j * tile, tile), tile)
        every = jnp.concatenate([ids[t][0:1, :] for t in range(S)], axis=1)
        onehot = (row_ids(j, tile, S * T) == every).astype(f32).astype(bf16)
        embed = 0.0
        for p in range(S // 2):
            embed = embed + over_tokens(onehot[:, 2 * p * T:2 * (p + 1) * T], cf[p])
        emb[rows, :] = embed * root
        return carry

    def embed_ready():
        for t in range(S):
            got(cm.at[t], cm_r.at[t])
            assemble(cf, cq, cm, t)

    tiles = R // tile
    close = apart < 3

    zero = jnp.zeros((1, T), f32)
    sums = (zero, zero)
    for k in range(steps):
        logits(k)
        logit_start(k)
        if k:
            logit_relay(k - 1)
        if k == 1:
            pass_cot(1, 0, 2)
        if k == 2:
            pass_cot(1, 2, S)
    pass_cot(2, 0, 2)
    sums = softmax_sums(0, sums)
    for k in range(1, steps - 2):
        sums = softmax_sums(k, sums)
    logit_relay(steps - 1)
    for k in range(steps - 2):
        code_start(k)
    pass_cot(2, 2, S)
    sums = softmax_sums(steps - 2, sums)
    code_start(steps - 2)
    total, pick = softmax_sums(steps - 1, sums)
    stat_tx[0:8, :] = jnp.broadcast_to(total, (8, T))
    stat_tx[8:16, :] = jnp.broadcast_to(pick, (8, T))
    for r in range(1, V):
        rc(stat_tx, stat_rx.at[v], st_s, st_r.at[v], (s, (v + r) % V)).start()
    stat_rx[v] = stat_tx[...]
    for r in range(1, S):
        t = (s + r) % S
        got(ids.at[t], id_r.at[t])
    code_relay(0)

    @pl.when(close)
    def _():
        embed_ready()
        lax.fori_loop(0, tiles // 2, embed_tile, 0)

    for r in range(1, V):
        u = (v + r) % V
        got(stat_rx.at[u], st_r.at[u])
    sums = stat_rx[0]
    for u in range(1, V):
        sums = sums + stat_rx[u]
    total = sums[0:1, :]
    loss[...] = jnp.log(total) - sums[8:9, :]
    gain = scale[...]
    info[s] = jnp.concatenate(
        [gain / total, jnp.broadcast_to(gain, (7, T))], axis=0
    )
    for r in range(1, S):
        t = s ^ r
        rc(info.at[s], info.at[s], in_s, in_r.at[s], (t, v)).start()
    code_start(steps - 1)

    def rows_term(t, part):
        return lax.dot_general(
            dl[t, part], slab[part], (((0,), (0,)), ((), ())), preferred_element_type=f32
        )

    def give(t, g):
        gt[t] = g.T
        block = gt.at[t, pl.ds(pl.multiple_of((1 - c) * W, 16), W)]
        rc(block, px_rx.at[t], px_s, px_r.at[t], (s, mate)).start()

    def term(t):
        give(t, rows_term(t, slice(0, R)))

    lead, rest = slice(0, W // 2), slice(W // 2, W)

    def fin_send(q, src, part):
        @pl.when(q != z)
        def _():
            rc(src, fin.at[z, part], f_s.at[q], f_r.at[z], (s, 2 * q + c)).start()

        @pl.when(q == z)
        def _():
            fin[z, part] = src[...]

    def pass_on(t):
        got(px_rx.at[t], px_r.at[t])
        kept = gt[t, pl.ds(pl.multiple_of(c * W, 16), W), :]
        gs[t] = (kept + px_rx[t]).astype(bf16)

    def pass_near(t):
        pass_on(t)
        rc(gs.at[t], zr.at[s], g_s.at[t], g_r.at[s], (t, v)).start()

    def pass_far():
        pass_on(far)

        @pl.when(z != s)
        def _():
            rc(gs.at[far, rest], zf.at[z], zf_s, zf_r.at[z], (s, 2 * s + c)).start()

        @pl.when(z == s)
        def _():
            zf[z] = gs[far, rest]

        rc(gs.at[far, lead], zr.at[s, lead], g_s.at[far], g_r.at[s], (far, v)).start()

    def gather_far():
        @pl.when(z == s)
        def _():
            for r in range(1, Z):
                u = (z + r) % Z
                got(zf.at[u], zf_r.at[u])
            acc = zf[0].astype(f32)
            for u in range(1, Z):
                acc = acc + zf[u].astype(f32)
            zsum[...] = acc.astype(bf16)
            rc(zsum, whole, zw_s, zw_r, (far, v)).start()

    for k in range(steps):
        grad(s, k)
    term(s)
    @pl.when(close)
    def _():
        lax.fori_loop(tiles // 2, tiles, embed_tile, 0)

    code_relay(1)
    for t in (nx, ny):
        info_got(t)

    def near_got(k):
        code_got(5 * k + 2, nx, low[k])
        code_got(5 * k + 3, ny, high[k])
        grad(nx, k)
        grad(ny, k)

    def far_got(k):
        code_got(5 * k + 4, far, slice(k * span, (k + 1) * span))
        grad(far, k)

    early, late = slice(0, (steps - 1) * span), slice((steps - 1) * span, R)

    def early_term(t, slot):
        gp[slot] = rows_term(t, early)

    def late_term(t, slot):
        give(t, gp[slot] + rows_term(t, late))

    near_got(0)
    pass_on(s)
    fin_send(s, gs.at[s], slice(0, W))
    near_got(1)
    code_relay(2)
    near_got(2)
    code_relay(3)
    info_got(far)
    early_term(nx, 0)
    early_term(ny, 1)
    near_got(3)
    late_term(nx, 0)
    late_term(ny, 1)
    far_got(0)
    far_got(1)
    pass_near(nx)
    far_got(2)
    pass_near(ny)
    early_term(far, 2)
    far_got(3)
    late_term(far, 2)

    def drain():
        for k in range(Z - 1):
            for f in range(shares):
                @pl.when((z < Z - 1) & (z - k >= 0))
                def _():
                    sent(hid.at[slices[f]], zr_s.at[k * shares + f])

                @pl.when((z > 0) & (z + k <= Z - 1))
                def _():
                    sent(hid.at[slices[f]], zl_s.at[k * shares + f])
        sent(hq.at[0:S - 1], pl_s)
        sent(hq, mt_s)
        for b in range(S):
            @pl.when((z >= s) & (z < Z - 1))
            def _():
                sent(cot, cr_s.at[b])

            @pl.when((z <= s) & (z > 0))
            def _():
                sent(cot, cl_s.at[b])

        @pl.when(s != z)
        def _():
            sent(cot, cp_s)
        sent(ids.at[0:S - 1], id_s)
        sent(info.at[0:S - 1], in_s)
        sent(rcv, rs_s)
        sent(cd.at[0:S - 1], ag_s)
        sent(stat_rx.at[0:V - 1], st_s)

    def fin_pass(q, part):
        got(zr.at[q, part], g_r.at[q])
        fin_send(q, zr.at[q, part], part)

    def tied_tile(j, carry):
        rows = pl.ds(pl.multiple_of(j * tile, tile), tile)
        head = emb[rows, :]
        for p in range(S // 2):
            lhs = jnp.concatenate([dl[2 * p, rows, :], dl[2 * p + 1, rows, :]], axis=1)
            head = head + over_tokens(lhs, h[p])
        tied[rows, :] = head.astype(bf16)
        return carry

    begun = tiles // 4
    drain()
    pass_far()

    @pl.when(jnp.logical_not(close))
    def _():
        for distance in range(3, Z):
            pass_cot(distance, 0, S)
        embed_ready()

    def late_embed(first, last):
        @pl.when(jnp.logical_not(close))
        def _():
            lax.fori_loop(first, last, embed_tile, 0)

    late_embed(0, tiles // 4)
    fin_pass(nx, slice(0, W))
    late_embed(tiles // 4, tiles * 3 // 4)
    fin_pass(ny, slice(0, W))
    late_embed(tiles * 3 // 4, tiles)
    fin_pass(far, lead)
    lax.fori_loop(0, begun, tied_tile, 0)
    gather_far()
    lax.fori_loop(begun, tiles, tied_tile, 0)

    def fin_sum(part):
        for r in range(1, Z):
            u = (z + r) % Z
            got(fin.at[u, part], f_r.at[u])
        acc = fin[0, part].astype(f32)
        for u in range(1, Z):
            acc = acc + fin[u, part].astype(f32)
        hgrad[part] = acc.astype(bf16)

    @pl.when(z == far)
    def _():
        fin_sum(lead)
        got(whole, zw_r)
        hgrad[rest] = whole[...]

    @pl.when(z != far)
    def _():
        fin_sum(slice(0, W))


    for r in range(1, S):
        part = lead if r == 3 else slice(0, W)
        sent(gs.at[0, part], g_s.at[s ^ r])
    for r in range(S):
        part = lead if r == 3 else slice(0, W)

        @pl.when(s ^ r != z)
        def _():
            sent(gs.at[0, part], f_s.at[s ^ r])

    sent(cq, cm_s)
    sent(px_rx, px_s)

    @pl.when(z != s)
    def _():
        sent(gs.at[0, rest], zf_s)

    @pl.when(z == s)
    def _():
        sent(zsum, zw_s)


def put_out(loss, hgrad, tied, loss_out, hgrad_out, tied_out, sems):
    count = sems.shape[0] - 2
    rows = tied.shape[0] // count
    pairs = [(tied.at[pl.ds(n * rows, rows)], tied_out.at[pl.ds(n * rows, rows)]) for n in range(count)]
    pairs += [(hgrad, hgrad_out), (loss, loss_out)]
    moves = [pltpu.make_async_copy(src, dst, sems.at[i]) for i, (src, dst) in enumerate(pairs)]
    for move in moves:
        move.start()
    for move in moves:
        move.wait()


def fused(hidden, slab, token_ids, target_ids, input_cot, loss_grad):
    S = lax.axis_size("section")
    V = lax.axis_size("vocab")
    Z = V // 2
    T, W = hidden.shape
    R, Q = slab.shape
    vm = pltpu.VMEM
    dma = pltpu.SemaphoreType.DMA
    half = vm((S, W, T), bf16)
    both = vm((S // 2, Q, 2 * T), bf16)
    scratch = [
        vm((W, T), bf16), vm((W, T), bf16),
        vm((1, T), jnp.int32), vm((1, T), jnp.int32), vm((1, T), f32),
        vm((R, Q), bf16), half, half, half, both,
        vm((S, R, T), jnp.int16), vm((3, R, T), jnp.int16), vm((R, T), f32),
        half, half, both, vm((S, 8, T), jnp.int32), vm((8, T), jnp.int32),
        vm((S, R, T), jnp.int16), vm((16, T), f32), vm((V, 16, T), f32),
        vm((S, 8, T), f32), vm((S, R, T), bf16), vm((3, T, Q), f32), vm((S, Q, T), f32), vm((S, W, T), f32), half, half, vm((Z, W, T), bf16),
        vm((Z, W // 2, T), bf16), vm((W // 2, T), bf16), vm((W // 2, T), bf16), vm((R, Q), f32),
        dma((6,)), *[dma((Z * shares,))] * 4,
        dma, dma((S * shares,)), dma, dma((S * shares,)), dma, dma((S,)),
        dma((S,)), dma((S,)), dma((S,)), dma, dma((S,)), dma, dma((S,)),
        dma, dma((S,)),
        dma, dma((3 * steps,)), dma, dma((V,)), dma, dma((5 * steps,)),
        dma, dma((S,)), dma((S,)), dma((S,)), dma((Z,)), dma((Z,)),
        dma, dma((Z,)), dma, dma,
    ]
    block = pl.BlockSpec(memory_space=vm)
    anywhere = pl.BlockSpec(memory_space=pl.ANY)
    far_memory = pl.BlockSpec(memory_space=pltpu.HBM)
    results = pl.pallas_call(
        functools.partial(fused_kernel, (S, V)),
        out_shape=(
            jax.ShapeDtypeStruct((1, T), f32),
            jax.ShapeDtypeStruct((W, T), bf16),
            jax.ShapeDtypeStruct((R, Q), bf16),
        ),
        in_specs=[far_memory] * 6,
        out_specs=(block, block, block),
        scratch_shapes=scratch,
        compiler_params=pltpu.CompilerParams(
            collective_id=0, has_side_effects=True, vmem_limit_bytes=48 * 2**20
        ),
        name="fused",
    )(
        *(
            pltpu.with_memory_space_constraint(x, pltpu.HBM)
            for x in (
                hidden.T, input_cot.T, slab,
                token_ids.reshape(1, T), target_ids.reshape(1, T), loss_grad.reshape(1, T),
            )
        )
    )
    loss, hgrad, tied = pl.pallas_call(
        put_out,
        out_shape=tuple(jax.ShapeDtypeStruct(x.shape, x.dtype) for x in results),
        in_specs=[block] * 3,
        out_specs=(anywhere,) * 3,
        scratch_shapes=[dma((10,))],
        compiler_params=pltpu.CompilerParams(vmem_limit_bytes=8 * 2**20),
        name="put_out",
    )(*results)
    return loss.reshape(T), hgrad.T, tied


def from_partner(block, axis, stride):
    count = lax.axis_size(axis)
    route = []
    for low in range(count):
        high = low | 1 << stride
        if high != low and high < count:
            route += [(low, high), (high, low)]
    return lax.ppermute(block, axis, route)


def left_product(left_side, right_side):
    return lax.dot_general(
        left_side, right_side, (((0,), (0,)), ((), ())), preferred_element_type=jnp.float32
    )


def local_parts(raw_logits, targets, columns):
    capped = logit_cap * jnp.tanh(raw_logits / logit_cap)
    exp_logits = jnp.exp(capped)
    target_hit = (targets[:, None] == columns[None, :]).astype(jnp.float32)
    local_total = jnp.sum(exp_logits, axis=1)
    local_pick = jnp.sum(target_hit * capped, axis=1)
    return (capped, exp_logits, target_hit, local_total, local_pick)


def finish(capped, exp_logits, target_hit, exp_total, picked, scales):
    token_loss = jnp.log(exp_total) - picked
    slope = 1.0 - (capped / logit_cap) ** 2
    dlogit = (scales[:, None] * (exp_logits / exp_total[:, None] - target_hit) * slope).astype(
        jnp.bfloat16
    )
    return (token_loss, dlogit)


def general(hidden, slab, token_ids, target_ids, input_cot, loss_grad):
    rows_here = slab.shape[0]
    quarter_width = slab.shape[1]
    sections = lax.axis_size("section")
    shards = lax.axis_size("vocab")
    model_width = quarter_width * sections
    own_tokens = hidden.shape[0]
    share_width = hidden.shape[1]
    full_hidden, full_cot = (
        lax.all_gather(hidden, "vocab", axis=1, tiled=True),
        lax.all_gather(input_cot, "vocab", axis=1, tiled=True),
    )
    hidden_part, cot_part = (
        lax.all_to_all(full_hidden, "section", split_axis=1, concat_axis=0, tiled=True),
        lax.all_to_all(full_cot, "section", split_axis=1, concat_axis=0, tiled=True),
    )
    partial_value = lax.dot_general(
        hidden_part, slab, (((1,), (1,)), ((), ())), preferred_element_type=jnp.float32
    )
    columns = lax.axis_index("vocab") * rows_here + jnp.arange(rows_here, dtype=jnp.int32)
    raw_logits = lax.psum_scatter(partial_value, "section", scatter_dimension=0, tiled=True)
    capped, exp_logits, target_hit, local_total, local_pick = local_parts(
        raw_logits, target_ids, columns
    )
    exp_total, picked = lax.psum((local_total, local_pick), "vocab")
    token_loss, dlogit = finish(capped, exp_logits, target_hit, exp_total, picked, loss_grad)
    all_ids = lax.all_gather(token_ids, "section", axis=0, tiled=True)
    all_dlogit = lax.all_gather(dlogit, "section", axis=0, tiled=True)
    total_tokens = all_dlogit.shape[0]
    blocks = shards // sections
    narrow = share_width // sections
    arranged_slab = slab.reshape(rows_here, blocks, sections, narrow)
    term = jnp.einsum(
        "tv,vkrw->trkw", all_dlogit, arranged_slab, preferred_element_type=jnp.float32
    )
    term = term.reshape(total_tokens, shards * narrow)
    piece = lax.psum_scatter(term, "vocab", scatter_dimension=1, tiled=True).astype(jnp.bfloat16)
    slots = lax.all_to_all(piece, "section", split_axis=0, concat_axis=0, tiled=True).reshape(
        sections, own_tokens, narrow
    )
    base_bit = blocks.bit_length() - 1
    rank_high = lax.axis_index("vocab") // blocks
    for level in range(sections.bit_length() - 1):
        span = 1 << level
        shaped = slots.reshape(sections // (2 * span), 2, span, own_tokens, narrow)
        mine_bit = rank_high // span % 2
        lower = shaped[:, 0]
        upper = shaped[:, 1]
        keep = jnp.where(mine_bit == 0, lower, upper)
        outgoing = jnp.where(mine_bit == 0, upper, lower)
        incoming = from_partner(outgoing, "vocab", base_bit + level)
        first = jnp.where(mine_bit == 0, keep, incoming)
        second = jnp.where(mine_bit == 0, incoming, keep)
        slots = jnp.stack([first, second], axis=1).reshape(sections, own_tokens, narrow)
    hidden_grad = jnp.transpose(slots, (1, 0, 2)).reshape(own_tokens, sections * narrow)
    onehot = (all_ids[:, None] == columns[None, :]).astype(jnp.bfloat16)
    embed_scale = math.sqrt(model_width)
    tied_grad = left_product(all_dlogit, hidden_part) + left_product(onehot, cot_part) * embed_scale
    return (token_loss, hidden_grad, tied_grad.astype(jnp.bfloat16))


def on_device(hidden, slab, token_ids, target_ids, input_cot, loss_grad):
    sections = lax.axis_size("section")
    shards = lax.axis_size("vocab")
    fits = (
        sections == 4
        and shards == 2 * sections
        and hidden.shape[0] % 128 == 0
        and slab.shape[0] % 2048 == 0
        and hidden.shape[1] % 32 == 0
    )
    step = fused if fits else general
    return step(hidden, slab, token_ids, target_ids, input_cot, loss_grad)


def solution(mesh):
    placed = (
        P("section", "vocab"),
        P("vocab", "section"),
        P("section"),
        P("section"),
        P("section", "vocab"),
        P("section"),
    )
    return jax.shard_map(
        on_device,
        mesh=mesh,
        in_specs=placed,
        out_specs=(P("section"), P("section", "vocab"), P("vocab", "section")),
        check_vma=False,
    )
```

```python
import functools
import math

import jax
import jax.numpy as jnp
from jax import lax
from jax.experimental import pallas as pl
from jax.experimental.pallas import tpu as pltpu
from jax.sharding import PartitionSpec as P

logit_cap = 30.0
code_knee = 16.0
code_top = 32767.0
f32 = jnp.float32
bf16 = jnp.bfloat16


eighths = (0, 1, 2, 4, 6, 8)
steps = len(eighths) - 1
shares = 2


def encode(x):
    y = x / (jnp.abs(x) + code_knee) * code_top
    return jnp.floor(y + 0.5).astype(jnp.int32).astype(jnp.int16)


def decode(code):
    y = code.astype(jnp.int32).astype(f32) * (1.0 / code_top)
    return code_knee * y / (1.0 - jnp.abs(y))


def over_tokens(left, right):
    return lax.dot_general(
        left, right, (((1,), (1,)), ((), ())), preferred_element_type=jnp.float32
    )


def fused_kernel(
    dims, hid_hbm, cot_hbm, slab_hbm, tok_hbm, tgt_hbm, scale_hbm, loss, hgrad, tied,
    hid, cot, tok, tgt, scale,
    slab, zg, hq, hm, h, snd, rcv, own, cq, cm, cf, ids, tid_tx, cd, stat_tx, stat_rx,
    info, dl, gp, gt, px_rx, gs, zr, fin, zf, zsum, whole, emb,
    in_sem, zr_s, zr_r, zl_s, zl_r, pl_s, pl_r, mt_s, mt_r, cp_s, cp_r, cr_s, cl_s, cz_r,
    cm_s, cm_r, id_s, id_r, in_s, in_r, rs_s, rs_r, st_s, st_r, ag_s, ag_r, px_s, px_r, g_s, g_r, f_s, f_r, zf_s, zf_r, zw_s, zw_r,
):
    S, V = dims
    Z = V // 2
    W, T = hid.shape
    R, Q = slab.shape
    edges = [R * n // 8 for n in eighths]
    spans = [slice(a, b) for a, b in zip(edges, edges[1:])]
    s = lax.axis_index("section")
    v = lax.axis_index("vocab")
    z = v // 2
    c = v % 2
    mate = z * 2 + 1 - c
    nx, ny, far = s ^ 1, s ^ 2, s ^ 3
    tile = 256

    def rc(src, dst, ssem, rsem, dev):
        return pltpu.make_async_remote_copy(
            src_ref=src, dst_ref=dst, send_sem=ssem, recv_sem=rsem,
            device_id=dev, device_id_type=pl.DeviceIdType.MESH,
        )

    def got(ref, rsem):
        rc(ref, ref, rsem, rsem, (s, mate)).wait_recv()

    def sent(ref, ssem):
        rc(ref, ref, ssem, ssem, (s, mate)).wait_send()

    loads = [
        pltpu.make_async_copy(src, dst, in_sem.at[i])
        for i, (src, dst) in enumerate(
            ((hid_hbm, hid), (cot_hbm, cot), (tok_hbm, tok), (tgt_hbm, tgt), (scale_hbm, scale), (slab_hbm, slab))
        )
    ]
    for load in loads:
        load.start()

    bar = pltpu.get_barrier_semaphore()
    for r in range(1, S):
        pl.semaphore_signal(bar, inc=1, device_id=((s + r) % S, v), device_id_type=pl.DeviceIdType.MESH)
    for r in range(1, V):
        pl.semaphore_signal(bar, inc=1, device_id=(s, (v + r) % V), device_id_type=pl.DeviceIdType.MESH)
    for load in loads[:5]:
        load.wait()
    both_ids = jnp.concatenate([jnp.broadcast_to(x[...], (4, T)) for x in (tok, tgt)], axis=0)
    tid_tx[...] = both_ids
    ids[s] = both_ids
    pl.semaphore_wait(bar, S + V - 2)

    piece = W // shares
    slices = [slice(f * piece, (f + 1) * piece) for f in range(shares)]

    def z_send(k, f):
        part = slices[f]
        n = k * shares + f
        b = z - k

        @pl.when((z < Z - 1) & (b >= 0))
        def _():
            src = hid.at[part] if k == 0 else zg.at[b, part]
            rc(src, zg.at[b, part], zr_s.at[n], zr_r.at[n], (s, v + 2)).start()

        d = z + k

        @pl.when((z > 0) & (d <= Z - 1))
        def _():
            src = hid.at[part] if k == 0 else zg.at[d, part]
            rc(src, zg.at[d, part], zl_s.at[n], zl_r.at[n], (s, v - 2)).start()

    def plane_send(b, src, f):
        part = slices[f]

        @pl.when(b != s)
        def _():
            rc(src, hq.at[s, part], pl_s, pl_r.at[s * shares + f], (b, v)).start()

        @pl.when(b == s)
        def _():
            n = s * shares + f
            rc(src, hm.at[s, part], mt_s, mt_r.at[n], (s, mate)).start()
            hq[s, part] = src[...]

    for f in range(shares):
        z_send(0, f)
    for f in range(shares):
        plane_send(z, hid.at[slices[f]], f)

    @pl.when(s != z)
    def _():
        rc(cot, cq.at[s], cp_s, cp_r.at[s], (z, v)).start()

    for r in range(1, S):
        t = (s + r) % S
        rc(tid_tx, ids.at[s], id_s, id_r.at[s], (t, v)).start()

    for k in range(Z - 1):
        b = z - 1 - k
        d = z + 1 + k
        for f in range(shares):
            part = slices[f]
            n = k * shares + f

            @pl.when(b >= 0)
            def _():
                got(zg.at[b, part], zr_r.at[n])

            @pl.when(d <= Z - 1)
            def _():
                got(zg.at[d, part], zl_r.at[n])

            if k + 1 < Z - 1:
                z_send(k + 1, f)

            @pl.when(b >= 0)
            def _():
                plane_send(b, zg.at[b, part], f)

            @pl.when(d <= Z - 1)
            def _():
                plane_send(d, zg.at[d, part], f)

    def forward(src, t):
        @pl.when((z >= s) & (z < Z - 1))
        def _():
            rc(src, cq.at[t], cr_s.at[t], cz_r.at[t], (s, v + 2)).start()

        @pl.when((z <= s) & (z > 0))
        def _():
            rc(src, cq.at[t], cl_s.at[t], cz_r.at[t], (s, v - 2)).start()

        rc(src, cm.at[t], cm_s, cm_r.at[t], (s, mate)).start()

    @pl.when(z == s)
    def _():
        cq[s] = cot[...]
        forward(cot, s)
        for r in range(1, S):
            t = (s + r) % S
            got(cq.at[t], cp_r.at[t])
            forward(cq.at[t], t)

    apart = jnp.abs(z - s)

    def pass_cot(distance, first, last):
        @pl.when(apart == distance)
        def _():
            for r in range(first, last):
                t = (s + r) % S
                got(cq.at[t], cz_r.at[t])
                forward(cq.at[t], t)

    for f in range(shares):
        for r in range(1, S):
            t = s ^ r
            n = t * shares + f
            got(hq.at[t, slices[f]], pl_r.at[n])
            rc(hq.at[t, slices[f]], hm.at[t, slices[f]], mt_s, mt_r.at[n], (s, mate)).start()

    def assemble(full, mine, other, t):
        cols = slice(t % 2 * T, (t % 2 + 1) * T)
        full[t // 2, pl.ds(pl.multiple_of(c * W, 16), W), cols] = mine[t]
        full[t // 2, pl.ds(pl.multiple_of((1 - c) * W, 16), W), cols] = other[t]

    for t in range(S):
        for f in range(shares):
            got(hm.at[t, slices[f]], mt_r.at[t * shares + f])
        assemble(h, hq, hm, t)
    loads[5].wait()

    low = [slice(x.start, (x.start + x.stop) // 2) for x in spans]
    high = [slice((x.start + x.stop) // 2, x.stop) for x in spans]
    other = 1 - s // 2
    even = s % 2 == 0

    def logits(k):
        def logit_tile(j, carry):
            rows = pl.ds(pl.multiple_of(j * tile, tile), tile)
            part = jnp.dot(slab[rows, :], h[other], preferred_element_type=f32)
            for m in range(2):
                snd[2 * other + m, rows, :] = encode(part[:, m * T:(m + 1) * T])
            part = jnp.dot(slab[rows, :], h[s // 2], preferred_element_type=f32)
            own[rows, :] = jnp.where(even, part[:, :T], part[:, T:])
            snd[nx, rows, :] = encode(jnp.where(even, part[:, T:], part[:, :T]))
            return carry

        lax.fori_loop(spans[k].start // tile, spans[k].stop // tile, logit_tile, 0)

    def logit_send(n, t, slot, part, to):
        rc(snd.at[t, part], rcv.at[slot, part], rs_s, rs_r.at[n], (to, v)).start()

    def logit_got(n, slot, part):
        got(rcv.at[slot, part], rs_r.at[n])

    def relay(t, part):
        def relay_tile(j, carry):
            rows = pl.ds(pl.multiple_of(j * soft, soft), soft)
            snd[t, rows, :] = encode(decode(snd[t, rows, :]) + decode(rcv[2, rows, :]))
            return carry

        lax.fori_loop(part.start // soft, part.stop // soft, relay_tile, 0)

    def logit_start(k):
        logit_send(3 * k, far, 2, low[k], nx)
        logit_send(3 * k + 1, far, 2, high[k], ny)
        logit_send(3 * k + 2, nx, 0, low[k], nx)
        logit_send(3 * k + 2, ny, 1, high[k], ny)

    def logit_relay(k):
        logit_got(3 * k, 2, low[k])
        relay(ny, low[k])
        logit_send(3 * k + 2, ny, 1, low[k], ny)
        logit_got(3 * k + 1, 2, high[k])
        relay(nx, high[k])
        logit_send(3 * k + 2, nx, 0, high[k], nx)

    soft = 128
    target = tgt[...]
    unit = logit_cap / code_top

    def row_ids(j, n, width):
        return v * R + j * n + lax.broadcasted_iota(jnp.int32, (n, width), 0)

    def softmax_sums(k, sums):
        logit_got(3 * k + 2, slice(0, 2), spans[k])

        def soft_tile(j, carry):
            total, pick = carry
            rows = pl.ds(pl.multiple_of(j * soft, soft), soft)
            raw = own[rows, :] + decode(rcv[0, rows, :]) + decode(rcv[1, rows, :])
            bent = jnp.tanh(raw / logit_cap)
            code = jnp.floor(bent * code_top + 0.5)
            cd[s, rows, :] = code.astype(jnp.int32).astype(jnp.int16)
            hit = row_ids(j, soft, T) == target
            total = total + jnp.sum(jnp.exp(code * unit), axis=0, keepdims=True)
            pick = pick + jnp.sum(jnp.where(hit, logit_cap * bent, 0.0), axis=0, keepdims=True)
            return total, pick

        return lax.fori_loop(spans[k].start // soft, spans[k].stop // soft, soft_tile, sums)

    def code_send(n, t, part, to):
        block = cd.at[t, part]
        rc(block, block, ag_s, ag_r.at[n], (to, v)).start()

    def code_got(n, t, part):
        got(cd.at[t, part], ag_r.at[n])

    def code_start(k):
        code_send(5 * k, s, high[k], nx)
        code_send(5 * k + 1, s, low[k], ny)
        code_send(5 * k + 2, s, low[k], nx)
        code_send(5 * k + 3, s, high[k], ny)

    def code_relay(k):
        code_got(5 * k + 1, ny, low[k])
        code_send(5 * k + 4, ny, low[k], nx)
        code_got(5 * k, nx, high[k])
        code_send(5 * k + 4, nx, high[k], ny)

    def info_got(t):
        got(info.at[t], in_r.at[t])

    def grad(t, k):
        scale_row = info[t][0:1, :]
        gain_row = info[t][1:2, :]
        target_row = ids[t][4:5, :]

        def grad_tile(j, carry):
            rows = pl.ds(pl.multiple_of(j * soft, soft), soft)
            code = cd[t, rows, :].astype(jnp.int32).astype(f32)
            hit = row_ids(j, soft, T) == target_row
            slope = 1.0 - (code * (1.0 / code_top)) ** 2
            away = jnp.exp(code * unit) * scale_row - jnp.where(hit, gain_row, 0.0)
            dl[t, rows, :] = (away * slope).astype(bf16)
            return carry

        lax.fori_loop(spans[k].start // soft, spans[k].stop // soft, grad_tile, 0)

    root = math.sqrt(Q * S)

    def embed_tile(j, carry):
        rows = pl.ds(pl.multiple_of(j * tile, tile), tile)
        every = jnp.concatenate([ids[t][0:1, :] for t in range(S)], axis=1)
        onehot = (row_ids(j, tile, S * T) == every).astype(f32).astype(bf16)
        embed = 0.0
        for p in range(S // 2):
            embed = embed + over_tokens(onehot[:, 2 * p * T:2 * (p + 1) * T], cf[p])
        emb[rows, :] = embed * root
        return carry

    def embed_ready():
        for t in range(S):
            got(cm.at[t], cm_r.at[t])
            assemble(cf, cq, cm, t)

    tiles = R // tile
    close = apart < 3

    zero = jnp.zeros((1, T), f32)
    sums = (zero, zero)
    for k in range(steps):
        logits(k)
        logit_start(k)
        if k > 1:
            logit_relay(k - 2)
        if k == 3:
            pass_cot(1, 0, 2)
        if k == 4:
            pass_cot(1, 2, S)
    logit_relay(steps - 2)
    pass_cot(2, 0, 2)
    for k in range(steps // 2):
        sums = softmax_sums(k, sums)
    logit_relay(steps - 1)
    for k in range(steps // 2):
        code_start(k)
    pass_cot(2, 2, S)
    for k in range(steps // 2, steps - 1):
        sums = softmax_sums(k, sums)
        code_start(k)
    total, pick = softmax_sums(steps - 1, sums)
    stat_tx[0:8, :] = jnp.broadcast_to(total, (8, T))
    stat_tx[8:16, :] = jnp.broadcast_to(pick, (8, T))
    for r in range(1, V):
        rc(stat_tx, stat_rx.at[v], st_s, st_r.at[v], (s, (v + r) % V)).start()
    stat_rx[v] = stat_tx[...]
    for r in range(1, S):
        t = (s + r) % S
        got(ids.at[t], id_r.at[t])
    code_relay(0)

    @pl.when(close)
    def _():
        embed_ready()
        lax.fori_loop(0, tiles // 2, embed_tile, 0)

    for r in range(1, V):
        u = (v + r) % V
        got(stat_rx.at[u], st_r.at[u])
    sums = stat_rx[0]
    for u in range(1, V):
        sums = sums + stat_rx[u]
    total = sums[0:1, :]
    loss[...] = jnp.log(total) - sums[8:9, :]
    gain = scale[...]
    info[s] = jnp.concatenate(
        [gain / total, jnp.broadcast_to(gain, (7, T))], axis=0
    )
    for r in range(1, S):
        t = s ^ r
        rc(info.at[s], info.at[s], in_s, in_r.at[s], (t, v)).start()
    code_start(steps - 1)

    def rows_term(t, part):
        return lax.dot_general(
            dl[t, part], slab[part], (((0,), (0,)), ((), ())), preferred_element_type=f32
        )

    def give(t, g):
        gt[t] = g.T
        block = gt.at[t, pl.ds(pl.multiple_of((1 - c) * W, 16), W)]
        rc(block, px_rx.at[t], px_s, px_r.at[t], (s, mate)).start()

    def term(t):
        give(t, rows_term(t, slice(0, R)))

    lead, rest = slice(0, W // 2), slice(W // 2, W)

    def fin_send(q, src, part):
        @pl.when(q != z)
        def _():
            rc(src, fin.at[z, part], f_s.at[q], f_r.at[z], (s, 2 * q + c)).start()

        @pl.when(q == z)
        def _():
            fin[z, part] = src[...]

    def pass_on(t):
        got(px_rx.at[t], px_r.at[t])
        kept = gt[t, pl.ds(pl.multiple_of(c * W, 16), W), :]
        gs[t] = (kept + px_rx[t]).astype(bf16)

    def pass_near(t):
        pass_on(t)
        rc(gs.at[t], zr.at[s], g_s.at[t], g_r.at[s], (t, v)).start()

    def pass_far():
        pass_on(far)

        @pl.when(z != s)
        def _():
            rc(gs.at[far, rest], zf.at[z], zf_s, zf_r.at[z], (s, 2 * s + c)).start()

        @pl.when(z == s)
        def _():
            zf[z] = gs[far, rest]

        rc(gs.at[far, lead], zr.at[s, lead], g_s.at[far], g_r.at[s], (far, v)).start()

    def gather_far():
        @pl.when(z == s)
        def _():
            for r in range(1, Z):
                u = (z + r) % Z
                got(zf.at[u], zf_r.at[u])
            acc = zf[0].astype(f32)
            for u in range(1, Z):
                acc = acc + zf[u].astype(f32)
            zsum[...] = acc.astype(bf16)
            rc(zsum, whole, zw_s, zw_r, (far, v)).start()

    for k in range(steps):
        grad(s, k)
    term(s)
    @pl.when(close)
    def _():
        lax.fori_loop(tiles // 2, tiles, embed_tile, 0)

    code_relay(1)
    code_relay(2)
    for t in (nx, ny):
        info_got(t)

    def near_got(k):
        code_got(5 * k + 2, nx, low[k])
        code_got(5 * k + 3, ny, high[k])
        grad(nx, k)
        grad(ny, k)

    def far_got(k):
        code_got(5 * k + 4, far, spans[k])
        grad(far, k)

    early, late = slice(0, edges[-2]), spans[-1]

    def early_term(t, slot):
        gp[slot] = rows_term(t, early)

    def late_term(t, slot):
        give(t, gp[slot] + rows_term(t, late))

    near_got(0)
    pass_on(s)
    fin_send(s, gs.at[s], slice(0, W))
    for k in range(3, steps):
        near_got(k - 2)
        code_relay(k)
    for distance in range(3, Z):
        pass_cot(distance, 0, S)
    info_got(far)
    near_got(steps - 2)
    early_term(nx, 0)
    early_term(ny, 1)
    near_got(steps - 1)
    late_term(nx, 0)
    late_term(ny, 1)
    for k in range(steps // 2):
        far_got(k)
    pass_near(nx)
    for k in range(steps // 2, steps - 1):
        far_got(k)
    pass_near(ny)
    early_term(far, 2)
    far_got(steps - 1)
    late_term(far, 2)

    def drain():
        for k in range(Z - 1):
            for f in range(shares):
                @pl.when((z < Z - 1) & (z - k >= 0))
                def _():
                    sent(hid.at[slices[f]], zr_s.at[k * shares + f])

                @pl.when((z > 0) & (z + k <= Z - 1))
                def _():
                    sent(hid.at[slices[f]], zl_s.at[k * shares + f])
        sent(hq.at[0:S - 1], pl_s)
        sent(hq, mt_s)
        for b in range(S):
            @pl.when((z >= s) & (z < Z - 1))
            def _():
                sent(cot, cr_s.at[b])

            @pl.when((z <= s) & (z > 0))
            def _():
                sent(cot, cl_s.at[b])

        @pl.when(s != z)
        def _():
            sent(cot, cp_s)
        sent(ids.at[0:S - 1], id_s)
        sent(info.at[0:S - 1], in_s)
        sent(rcv, rs_s)
        sent(cd.at[0:S - 1], ag_s)
        sent(stat_rx.at[0:V - 1], st_s)

    def fin_pass(q, part):
        got(zr.at[q, part], g_r.at[q])
        fin_send(q, zr.at[q, part], part)

    def tied_tile(j, carry):
        rows = pl.ds(pl.multiple_of(j * tile, tile), tile)
        head = emb[rows, :]
        for p in range(S // 2):
            lhs = jnp.concatenate([dl[2 * p, rows, :], dl[2 * p + 1, rows, :]], axis=1)
            head = head + over_tokens(lhs, h[p])
        tied[rows, :] = head.astype(bf16)
        return carry

    begun = tiles // 4
    drain()
    pass_far()

    @pl.when(jnp.logical_not(close))
    def _():
        embed_ready()

    def late_embed(first, last):
        @pl.when(jnp.logical_not(close))
        def _():
            lax.fori_loop(first, last, embed_tile, 0)

    late_embed(0, tiles // 4)
    fin_pass(nx, slice(0, W))
    late_embed(tiles // 4, tiles * 3 // 4)
    fin_pass(ny, slice(0, W))
    late_embed(tiles * 3 // 4, tiles)
    fin_pass(far, lead)
    lax.fori_loop(0, begun, tied_tile, 0)
    gather_far()
    lax.fori_loop(begun, tiles, tied_tile, 0)

    def fin_sum(part):
        for r in range(1, Z):
            u = (z + r) % Z
            got(fin.at[u, part], f_r.at[u])
        acc = fin[0, part].astype(f32)
        for u in range(1, Z):
            acc = acc + fin[u, part].astype(f32)
        hgrad[part] = acc.astype(bf16)

    @pl.when(z == far)
    def _():
        fin_sum(lead)
        got(whole, zw_r)
        hgrad[rest] = whole[...]

    @pl.when(z != far)
    def _():
        fin_sum(slice(0, W))


    for r in range(1, S):
        part = lead if r == 3 else slice(0, W)
        sent(gs.at[0, part], g_s.at[s ^ r])
    for r in range(S):
        part = lead if r == 3 else slice(0, W)

        @pl.when(s ^ r != z)
        def _():
            sent(gs.at[0, part], f_s.at[s ^ r])

    sent(cq, cm_s)
    sent(px_rx, px_s)

    @pl.when(z != s)
    def _():
        sent(gs.at[0, rest], zf_s)

    @pl.when(z == s)
    def _():
        sent(zsum, zw_s)


def put_out(loss, hgrad, tied, loss_out, hgrad_out, tied_out, sems):
    count = sems.shape[0] - 2
    rows = tied.shape[0] // count
    pairs = [(tied.at[pl.ds(n * rows, rows)], tied_out.at[pl.ds(n * rows, rows)]) for n in range(count)]
    pairs += [(hgrad, hgrad_out), (loss, loss_out)]
    moves = [pltpu.make_async_copy(src, dst, sems.at[i]) for i, (src, dst) in enumerate(pairs)]
    for move in moves:
        move.start()
    for move in moves:
        move.wait()


def fused(hidden, slab, token_ids, target_ids, input_cot, loss_grad):
    S = lax.axis_size("section")
    V = lax.axis_size("vocab")
    Z = V // 2
    T, W = hidden.shape
    R, Q = slab.shape
    vm = pltpu.VMEM
    dma = pltpu.SemaphoreType.DMA
    half = vm((S, W, T), bf16)
    both = vm((S // 2, Q, 2 * T), bf16)
    scratch = [
        vm((W, T), bf16), vm((W, T), bf16),
        vm((1, T), jnp.int32), vm((1, T), jnp.int32), vm((1, T), f32),
        vm((R, Q), bf16), half, half, half, both,
        vm((S, R, T), jnp.int16), vm((3, R, T), jnp.int16), vm((R, T), f32),
        half, half, both, vm((S, 8, T), jnp.int32), vm((8, T), jnp.int32),
        vm((S, R, T), jnp.int16), vm((16, T), f32), vm((V, 16, T), f32),
        vm((S, 8, T), f32), vm((S, R, T), bf16), vm((3, T, Q), f32), vm((S, Q, T), f32), vm((S, W, T), f32), half, half, vm((Z, W, T), bf16),
        vm((Z, W // 2, T), bf16), vm((W // 2, T), bf16), vm((W // 2, T), bf16), vm((R, Q), f32),
        dma((6,)), *[dma((Z * shares,))] * 4,
        dma, dma((S * shares,)), dma, dma((S * shares,)), dma, dma((S,)),
        dma((S,)), dma((S,)), dma((S,)), dma, dma((S,)), dma, dma((S,)),
        dma, dma((S,)),
        dma, dma((3 * steps,)), dma, dma((V,)), dma, dma((5 * steps,)),
        dma, dma((S,)), dma((S,)), dma((S,)), dma((Z,)), dma((Z,)),
        dma, dma((Z,)), dma, dma,
    ]
    block = pl.BlockSpec(memory_space=vm)
    anywhere = pl.BlockSpec(memory_space=pl.ANY)
    far_memory = pl.BlockSpec(memory_space=pltpu.HBM)
    results = pl.pallas_call(
        functools.partial(fused_kernel, (S, V)),
        out_shape=(
            jax.ShapeDtypeStruct((1, T), f32),
            jax.ShapeDtypeStruct((W, T), bf16),
            jax.ShapeDtypeStruct((R, Q), bf16),
        ),
        in_specs=[far_memory] * 6,
        out_specs=(block, block, block),
        scratch_shapes=scratch,
        compiler_params=pltpu.CompilerParams(
            collective_id=0, has_side_effects=True, vmem_limit_bytes=48 * 2**20
        ),
        name="fused",
    )(
        *(
            pltpu.with_memory_space_constraint(x, pltpu.HBM)
            for x in (
                hidden.T, input_cot.T, slab,
                token_ids.reshape(1, T), target_ids.reshape(1, T), loss_grad.reshape(1, T),
            )
        )
    )
    loss, hgrad, tied = pl.pallas_call(
        put_out,
        out_shape=tuple(jax.ShapeDtypeStruct(x.shape, x.dtype) for x in results),
        in_specs=[block] * 3,
        out_specs=(anywhere,) * 3,
        scratch_shapes=[dma((10,))],
        compiler_params=pltpu.CompilerParams(vmem_limit_bytes=8 * 2**20),
        name="put_out",
    )(*results)
    return loss.reshape(T), hgrad.T, tied


def from_partner(block, axis, stride):
    count = lax.axis_size(axis)
    route = []
    for low in range(count):
        high = low | 1 << stride
        if high != low and high < count:
            route += [(low, high), (high, low)]
    return lax.ppermute(block, axis, route)


def left_product(left_side, right_side):
    return lax.dot_general(
        left_side, right_side, (((0,), (0,)), ((), ())), preferred_element_type=jnp.float32
    )


def local_parts(raw_logits, targets, columns):
    capped = logit_cap * jnp.tanh(raw_logits / logit_cap)
    exp_logits = jnp.exp(capped)
    target_hit = (targets[:, None] == columns[None, :]).astype(jnp.float32)
    local_total = jnp.sum(exp_logits, axis=1)
    local_pick = jnp.sum(target_hit * capped, axis=1)
    return (capped, exp_logits, target_hit, local_total, local_pick)


def finish(capped, exp_logits, target_hit, exp_total, picked, scales):
    token_loss = jnp.log(exp_total) - picked
    slope = 1.0 - (capped / logit_cap) ** 2
    dlogit = (scales[:, None] * (exp_logits / exp_total[:, None] - target_hit) * slope).astype(
        jnp.bfloat16
    )
    return (token_loss, dlogit)


def general(hidden, slab, token_ids, target_ids, input_cot, loss_grad):
    rows_here = slab.shape[0]
    quarter_width = slab.shape[1]
    sections = lax.axis_size("section")
    shards = lax.axis_size("vocab")
    model_width = quarter_width * sections
    own_tokens = hidden.shape[0]
    share_width = hidden.shape[1]
    full_hidden, full_cot = (
        lax.all_gather(hidden, "vocab", axis=1, tiled=True),
        lax.all_gather(input_cot, "vocab", axis=1, tiled=True),
    )
    hidden_part, cot_part = (
        lax.all_to_all(full_hidden, "section", split_axis=1, concat_axis=0, tiled=True),
        lax.all_to_all(full_cot, "section", split_axis=1, concat_axis=0, tiled=True),
    )
    partial_value = lax.dot_general(
        hidden_part, slab, (((1,), (1,)), ((), ())), preferred_element_type=jnp.float32
    )
    columns = lax.axis_index("vocab") * rows_here + jnp.arange(rows_here, dtype=jnp.int32)
    raw_logits = lax.psum_scatter(partial_value, "section", scatter_dimension=0, tiled=True)
    capped, exp_logits, target_hit, local_total, local_pick = local_parts(
        raw_logits, target_ids, columns
    )
    exp_total, picked = lax.psum((local_total, local_pick), "vocab")
    token_loss, dlogit = finish(capped, exp_logits, target_hit, exp_total, picked, loss_grad)
    all_ids = lax.all_gather(token_ids, "section", axis=0, tiled=True)
    all_dlogit = lax.all_gather(dlogit, "section", axis=0, tiled=True)
    total_tokens = all_dlogit.shape[0]
    blocks = shards // sections
    narrow = share_width // sections
    arranged_slab = slab.reshape(rows_here, blocks, sections, narrow)
    term = jnp.einsum(
        "tv,vkrw->trkw", all_dlogit, arranged_slab, preferred_element_type=jnp.float32
    )
    term = term.reshape(total_tokens, shards * narrow)
    piece = lax.psum_scatter(term, "vocab", scatter_dimension=1, tiled=True).astype(jnp.bfloat16)
    slots = lax.all_to_all(piece, "section", split_axis=0, concat_axis=0, tiled=True).reshape(
        sections, own_tokens, narrow
    )
    base_bit = blocks.bit_length() - 1
    rank_high = lax.axis_index("vocab") // blocks
    for level in range(sections.bit_length() - 1):
        span = 1 << level
        shaped = slots.reshape(sections // (2 * span), 2, span, own_tokens, narrow)
        mine_bit = rank_high // span % 2
        lower = shaped[:, 0]
        upper = shaped[:, 1]
        keep = jnp.where(mine_bit == 0, lower, upper)
        outgoing = jnp.where(mine_bit == 0, upper, lower)
        incoming = from_partner(outgoing, "vocab", base_bit + level)
        first = jnp.where(mine_bit == 0, keep, incoming)
        second = jnp.where(mine_bit == 0, incoming, keep)
        slots = jnp.stack([first, second], axis=1).reshape(sections, own_tokens, narrow)
    hidden_grad = jnp.transpose(slots, (1, 0, 2)).reshape(own_tokens, sections * narrow)
    onehot = (all_ids[:, None] == columns[None, :]).astype(jnp.bfloat16)
    embed_scale = math.sqrt(model_width)
    tied_grad = left_product(all_dlogit, hidden_part) + left_product(onehot, cot_part) * embed_scale
    return (token_loss, hidden_grad, tied_grad.astype(jnp.bfloat16))


def on_device(hidden, slab, token_ids, target_ids, input_cot, loss_grad):
    sections = lax.axis_size("section")
    shards = lax.axis_size("vocab")
    fits = (
        sections == 4
        and shards == 2 * sections
        and hidden.shape[0] % 128 == 0
        and slab.shape[0] % 2048 == 0
        and hidden.shape[1] % 32 == 0
    )
    step = fused if fits else general
    return step(hidden, slab, token_ids, target_ids, input_cot, loss_grad)


def solution(mesh):
    placed = (
        P("section", "vocab"),
        P("vocab", "section"),
        P("section"),
        P("section"),
        P("section", "vocab"),
        P("section"),
    )
    return jax.shard_map(
        on_device,
        mesh=mesh,
        in_specs=placed,
        out_specs=(P("section"), P("section", "vocab"), P("vocab", "section")),
        check_vma=False,
    )
```

```python
import functools
import math

import jax
import jax.numpy as jnp
from jax import lax
from jax.experimental import pallas as pl
from jax.experimental.pallas import tpu as pltpu
from jax.sharding import PartitionSpec as P

logit_cap = 30.0
code_knee = 16.0
code_top = 32767.0
f32 = jnp.float32
bf16 = jnp.bfloat16


eighths = (0, 1, 2, 4, 6, 8)
steps = len(eighths) - 1
shares = 2


def encode(x):
    y = x / (jnp.abs(x) + code_knee) * code_top
    return jnp.floor(y + 0.5).astype(jnp.int32).astype(jnp.int16)


def decode(code):
    y = code.astype(jnp.int32).astype(f32) * (1.0 / code_top)
    return code_knee * y / (1.0 - jnp.abs(y))


def over_tokens(left, right):
    return lax.dot_general(
        left, right, (((1,), (1,)), ((), ())), preferred_element_type=jnp.float32
    )


def fused_kernel(
    dims, hid_hbm, cot_hbm, slab_hbm, tok_hbm, tgt_hbm, scale_hbm, loss, hgrad, tied,
    hid, cot, tok, tgt, scale,
    slab, zg, hq, hm, h, snd, rcv, own, cq, cm, cf, ids, tid_tx, cd, stat_tx, stat_rx,
    info, dl, gp, gt, px_rx, gs, zr, fin, zf, zsum, whole, emb,
    in_sem, zr_s, zr_r, zl_s, zl_r, pl_s, pl_r, mt_s, mt_r, cp_s, cp_r, cr_s, cl_s, cz_r,
    cm_s, cm_r, id_s, id_r, in_s, in_r, rs_s, rs_r, st_s, st_r, ag_s, ag_r, px_s, px_r, g_s, g_r, f_s, f_r, zf_s, zf_r, zw_s, zw_r,
):
    S, V = dims
    Z = V // 2
    W, T = hid.shape
    R, Q = slab.shape
    edges = [R * n // 8 for n in eighths]
    spans = [slice(a, b) for a, b in zip(edges, edges[1:])]
    s = lax.axis_index("section")
    v = lax.axis_index("vocab")
    z = v // 2
    c = v % 2
    mate = z * 2 + 1 - c
    nx, ny, far = s ^ 1, s ^ 2, s ^ 3
    tile = 256

    def rc(src, dst, ssem, rsem, dev):
        return pltpu.make_async_remote_copy(
            src_ref=src, dst_ref=dst, send_sem=ssem, recv_sem=rsem,
            device_id=dev, device_id_type=pl.DeviceIdType.MESH,
        )

    def got(ref, rsem):
        rc(ref, ref, rsem, rsem, (s, mate)).wait_recv()

    def sent(ref, ssem):
        rc(ref, ref, ssem, ssem, (s, mate)).wait_send()

    loads = [
        pltpu.make_async_copy(src, dst, in_sem.at[i])
        for i, (src, dst) in enumerate(
            ((hid_hbm, hid), (cot_hbm, cot), (tok_hbm, tok), (tgt_hbm, tgt), (scale_hbm, scale), (slab_hbm, slab))
        )
    ]
    for load in loads:
        load.start()

    bar = pltpu.get_barrier_semaphore()
    for r in range(1, S):
        pl.semaphore_signal(bar, inc=1, device_id=((s + r) % S, v), device_id_type=pl.DeviceIdType.MESH)
    for r in range(1, V):
        pl.semaphore_signal(bar, inc=1, device_id=(s, (v + r) % V), device_id_type=pl.DeviceIdType.MESH)
    for load in loads[:5]:
        load.wait()
    both_ids = jnp.concatenate([jnp.broadcast_to(x[...], (4, T)) for x in (tok, tgt)], axis=0)
    tid_tx[...] = both_ids
    ids[s] = both_ids
    pl.semaphore_wait(bar, S + V - 2)

    piece = W // shares
    slices = [slice(f * piece, (f + 1) * piece) for f in range(shares)]

    def z_send(k, f):
        part = slices[f]
        n = k * shares + f
        b = z - k

        @pl.when((z < Z - 1) & (b >= 0))
        def _():
            src = hid.at[part] if k == 0 else zg.at[b, part]
            rc(src, zg.at[b, part], zr_s.at[n], zr_r.at[n], (s, v + 2)).start()

        d = z + k

        @pl.when((z > 0) & (d <= Z - 1))
        def _():
            src = hid.at[part] if k == 0 else zg.at[d, part]
            rc(src, zg.at[d, part], zl_s.at[n], zl_r.at[n], (s, v - 2)).start()

    def plane_send(b, src, f):
        part = slices[f]

        @pl.when(b != s)
        def _():
            rc(src, hq.at[s, part], pl_s, pl_r.at[s * shares + f], (b, v)).start()

        @pl.when(b == s)
        def _():
            n = s * shares + f
            rc(src, hm.at[s, part], mt_s, mt_r.at[n], (s, mate)).start()
            hq[s, part] = src[...]

    for f in range(shares):
        z_send(0, f)
    for f in range(shares):
        plane_send(z, hid.at[slices[f]], f)

    @pl.when(s != z)
    def _():
        rc(cot, cq.at[s], cp_s, cp_r.at[s], (z, v)).start()

    for r in range(1, S):
        t = (s + r) % S
        rc(tid_tx, ids.at[s], id_s, id_r, (t, v)).start()

    for k in range(Z - 1):
        b = z - 1 - k
        d = z + 1 + k
        for f in range(shares):
            part = slices[f]
            n = k * shares + f

            @pl.when(b >= 0)
            def _():
                got(zg.at[b, part], zr_r.at[n])

            @pl.when(d <= Z - 1)
            def _():
                got(zg.at[d, part], zl_r.at[n])

            if k + 1 < Z - 1:
                z_send(k + 1, f)

            @pl.when(b >= 0)
            def _():
                plane_send(b, zg.at[b, part], f)

            @pl.when(d <= Z - 1)
            def _():
                plane_send(d, zg.at[d, part], f)

    def forward(src, t):
        @pl.when((z >= s) & (z < Z - 1))
        def _():
            rc(src, cq.at[t], cr_s.at[t], cz_r.at[t], (s, v + 2)).start()

        @pl.when((z <= s) & (z > 0))
        def _():
            rc(src, cq.at[t], cl_s.at[t], cz_r.at[t], (s, v - 2)).start()

        rc(src, cm.at[t], cm_s, cm_r, (s, mate)).start()

    @pl.when(z == s)
    def _():
        cq[s] = cot[...]
        forward(cot, s)
        for r in range(1, S):
            t = (s + r) % S
            got(cq.at[t], cp_r.at[t])
            forward(cq.at[t], t)

    apart = jnp.abs(z - s)

    def pass_cot(distance, first, last):
        @pl.when(apart == distance)
        def _():
            for r in range(first, last):
                t = (s + r) % S
                got(cq.at[t], cz_r.at[t])
                forward(cq.at[t], t)

    for f in range(shares):
        for r in range(1, S):
            t = s ^ r
            n = t * shares + f
            got(hq.at[t, slices[f]], pl_r.at[n])
            rc(hq.at[t, slices[f]], hm.at[t, slices[f]], mt_s, mt_r.at[n], (s, mate)).start()

    def assemble(full, mine, other, t):
        cols = slice(t % 2 * T, (t % 2 + 1) * T)
        full[t // 2, pl.ds(pl.multiple_of(c * W, 16), W), cols] = mine[t]
        full[t // 2, pl.ds(pl.multiple_of((1 - c) * W, 16), W), cols] = other[t]

    for t in range(S):
        for f in range(shares):
            got(hm.at[t, slices[f]], mt_r.at[t * shares + f])
        assemble(h, hq, hm, t)
    loads[5].wait()

    low = [slice(x.start, (x.start + x.stop) // 2) for x in spans]
    high = [slice((x.start + x.stop) // 2, x.stop) for x in spans]
    other = 1 - s // 2
    even = s % 2 == 0

    def logits(k):
        def logit_tile(j, carry):
            rows = pl.ds(pl.multiple_of(j * tile, tile), tile)
            part = jnp.dot(slab[rows, :], h[other], preferred_element_type=f32)
            for m in range(2):
                snd[2 * other + m, rows, :] = encode(part[:, m * T:(m + 1) * T])
            part = jnp.dot(slab[rows, :], h[s // 2], preferred_element_type=f32)
            own[rows, :] = jnp.where(even, part[:, :T], part[:, T:])
            snd[nx, rows, :] = encode(jnp.where(even, part[:, T:], part[:, :T]))
            return carry

        lax.fori_loop(spans[k].start // tile, spans[k].stop // tile, logit_tile, 0)

    def logit_send(n, t, slot, part, to):
        rc(snd.at[t, part], rcv.at[slot, part], rs_s, rs_r.at[n], (to, v)).start()

    def logit_got(n, slot, part):
        got(rcv.at[slot, part], rs_r.at[n])

    def relay(t, part):
        def relay_tile(j, carry):
            rows = pl.ds(pl.multiple_of(j * soft, soft), soft)
            snd[t, rows, :] = encode(decode(snd[t, rows, :]) + decode(rcv[2, rows, :]))
            return carry

        lax.fori_loop(part.start // soft, part.stop // soft, relay_tile, 0)

    def logit_start(k):
        logit_send(3 * k, far, 2, low[k], nx)
        logit_send(3 * k + 1, far, 2, high[k], ny)
        logit_send(3 * k + 2, nx, 0, low[k], nx)
        logit_send(3 * k + 2, ny, 1, high[k], ny)

    def logit_relay(k):
        logit_got(3 * k, 2, low[k])
        relay(ny, low[k])
        logit_send(3 * k + 2, ny, 1, low[k], ny)
        logit_got(3 * k + 1, 2, high[k])
        relay(nx, high[k])
        logit_send(3 * k + 2, nx, 0, high[k], nx)

    soft = 128
    target = tgt[...]
    unit = logit_cap / code_top

    def row_ids(j, n, width):
        return v * R + j * n + lax.broadcasted_iota(jnp.int32, (n, width), 0)

    def softmax_sums(k, sums):
        logit_got(3 * k + 2, slice(0, 2), spans[k])

        def soft_tile(j, carry):
            total, pick = carry
            rows = pl.ds(pl.multiple_of(j * soft, soft), soft)
            raw = own[rows, :] + decode(rcv[0, rows, :]) + decode(rcv[1, rows, :])
            bent = jnp.tanh(raw / logit_cap)
            code = jnp.floor(bent * code_top + 0.5)
            cd[s, rows, :] = code.astype(jnp.int32).astype(jnp.int16)
            hit = row_ids(j, soft, T) == target
            total = total + jnp.sum(jnp.exp(code * unit), axis=0, keepdims=True)
            pick = pick + jnp.sum(jnp.where(hit, logit_cap * bent, 0.0), axis=0, keepdims=True)
            return total, pick

        return lax.fori_loop(spans[k].start // soft, spans[k].stop // soft, soft_tile, sums)

    def code_send(n, t, part, to):
        block = cd.at[t, part]
        rc(block, block, ag_s, ag_r.at[n], (to, v)).start()

    def code_got(n, t, part):
        got(cd.at[t, part], ag_r.at[n])

    def code_start(k):
        code_send(5 * k, s, high[k], nx)
        code_send(5 * k + 1, s, low[k], ny)
        code_send(5 * k + 2, s, low[k], nx)
        code_send(5 * k + 3, s, high[k], ny)

    def code_relay(k):
        code_got(5 * k + 1, ny, low[k])
        code_send(5 * k + 4, ny, low[k], nx)
        code_got(5 * k, nx, high[k])
        code_send(5 * k + 4, nx, high[k], ny)

    def info_got(t):
        got(info.at[t], in_r.at[t])

    def grad(t, k):
        scale_row = info[t][0:1, :]
        gain_row = info[t][1:2, :]
        target_row = ids[t][4:5, :]

        def grad_tile(j, carry):
            rows = pl.ds(pl.multiple_of(j * soft, soft), soft)
            code = cd[t, rows, :].astype(jnp.int32).astype(f32)
            hit = row_ids(j, soft, T) == target_row
            slope = 1.0 - (code * (1.0 / code_top)) ** 2
            away = jnp.exp(code * unit) * scale_row - jnp.where(hit, gain_row, 0.0)
            dl[t, rows, :] = (away * slope).astype(bf16)
            return carry

        lax.fori_loop(spans[k].start // soft, spans[k].stop // soft, grad_tile, 0)

    root = math.sqrt(Q * S)

    def embed_tile(j, carry):
        rows = pl.ds(pl.multiple_of(j * tile, tile), tile)
        every = jnp.concatenate([ids[t][0:1, :] for t in range(S)], axis=1)
        onehot = (row_ids(j, tile, S * T) == every).astype(f32).astype(bf16)
        embed = 0.0
        for p in range(S // 2):
            embed = embed + over_tokens(onehot[:, 2 * p * T:2 * (p + 1) * T], cf[p])
        emb[rows, :] = embed * root
        return carry

    def embed_ready():
        got(cm, cm_r)
        for t in range(S):
            assemble(cf, cq, cm, t)

    tiles = R // tile
    close = apart < 3

    zero = jnp.zeros((1, T), f32)
    sums = (zero, zero)
    for k in range(steps):
        logits(k)
        logit_start(k)
        if k > 1:
            logit_relay(k - 2)
        if k == 3:
            pass_cot(1, 0, 2)
        if k == 4:
            pass_cot(1, 2, S)
    logit_relay(steps - 2)
    pass_cot(2, 0, 2)
    for k in range(steps // 2):
        sums = softmax_sums(k, sums)
    logit_relay(steps - 1)
    for k in range(steps // 2):
        code_start(k)
    pass_cot(2, 2, S)
    for k in range(steps // 2, steps - 1):
        sums = softmax_sums(k, sums)
        code_start(k)
    total, pick = softmax_sums(steps - 1, sums)
    stat_tx[0:8, :] = jnp.broadcast_to(total, (8, T))
    stat_tx[8:16, :] = jnp.broadcast_to(pick, (8, T))
    for r in range(1, V):
        rc(stat_tx, stat_rx.at[v], st_s, st_r, (s, (v + r) % V)).start()
    stat_rx[v] = stat_tx[...]
    got(ids.at[0:S - 1], id_r)
    code_relay(0)

    @pl.when(close)
    def _():
        embed_ready()
        lax.fori_loop(0, tiles // 2, embed_tile, 0)

    got(stat_rx.at[0:V - 1], st_r)
    sums = stat_rx[0]
    for u in range(1, V):
        sums = sums + stat_rx[u]
    total = sums[0:1, :]
    loss[...] = jnp.log(total) - sums[8:9, :]
    gain = scale[...]
    info[s] = jnp.concatenate(
        [gain / total, jnp.broadcast_to(gain, (7, T))], axis=0
    )
    for r in range(1, S):
        t = s ^ r
        rc(info.at[s], info.at[s], in_s, in_r.at[s], (t, v)).start()
    code_start(steps - 1)

    def rows_term(t, part):
        return lax.dot_general(
            dl[t, part], slab[part], (((0,), (0,)), ((), ())), preferred_element_type=f32
        )

    def give(t, g):
        gt[t] = g.T
        block = gt.at[t, pl.ds(pl.multiple_of((1 - c) * W, 16), W)]
        rc(block, px_rx.at[t], px_s, px_r.at[t], (s, mate)).start()

    def term(t):
        give(t, rows_term(t, slice(0, R)))

    lead, rest = slice(0, W // 2), slice(W // 2, W)

    def fin_send(q, src, part):
        @pl.when(q != z)
        def _():
            rc(src, fin.at[z, part], f_s.at[q], f_r.at[z], (s, 2 * q + c)).start()

        @pl.when(q == z)
        def _():
            fin[z, part] = src[...]

    def pass_on(t):
        got(px_rx.at[t], px_r.at[t])
        kept = gt[t, pl.ds(pl.multiple_of(c * W, 16), W), :]
        gs[t] = (kept + px_rx[t]).astype(bf16)

    def pass_near(t):
        pass_on(t)
        rc(gs.at[t], zr.at[s], g_s.at[t], g_r.at[s], (t, v)).start()

    def pass_far():
        pass_on(far)

        @pl.when(z != s)
        def _():
            rc(gs.at[far, rest], zf.at[z], zf_s, zf_r.at[z], (s, 2 * s + c)).start()

        @pl.when(z == s)
        def _():
            zf[z] = gs[far, rest]

        rc(gs.at[far, lead], zr.at[s, lead], g_s.at[far], g_r.at[s], (far, v)).start()

    def gather_far():
        @pl.when(z == s)
        def _():
            for r in range(1, Z):
                u = (z + r) % Z
                got(zf.at[u], zf_r.at[u])
            acc = zf[0].astype(f32)
            for u in range(1, Z):
                acc = acc + zf[u].astype(f32)
            zsum[...] = acc.astype(bf16)
            rc(zsum, whole, zw_s, zw_r, (far, v)).start()

    for k in range(steps):
        grad(s, k)
    term(s)
    @pl.when(close)
    def _():
        lax.fori_loop(tiles // 2, tiles, embed_tile, 0)

    code_relay(1)
    code_relay(2)
    for t in (nx, ny):
        info_got(t)

    def near_got(k):
        code_got(5 * k + 2, nx, low[k])
        code_got(5 * k + 3, ny, high[k])
        grad(nx, k)
        grad(ny, k)

    def far_got(k):
        code_got(5 * k + 4, far, spans[k])
        grad(far, k)

    early, late = slice(0, edges[-2]), spans[-1]

    def early_term(t, slot):
        gp[slot] = rows_term(t, early)

    def late_term(t, slot):
        give(t, gp[slot] + rows_term(t, late))

    near_got(0)
    pass_on(s)
    fin_send(s, gs.at[s], slice(0, W))
    for k in range(3, steps):
        near_got(k - 2)
        code_relay(k)
    for distance in range(3, Z):
        pass_cot(distance, 0, S)
    info_got(far)
    near_got(steps - 2)
    early_term(nx, 0)
    early_term(ny, 1)
    near_got(steps - 1)
    late_term(nx, 0)
    late_term(ny, 1)
    for k in range(steps // 2):
        far_got(k)
    pass_near(nx)
    for k in range(steps // 2, steps - 1):
        far_got(k)
    pass_near(ny)
    early_term(far, 2)
    far_got(steps - 1)
    late_term(far, 2)

    def drain():
        for k in range(Z - 1):
            for f in range(shares):
                @pl.when((z < Z - 1) & (z - k >= 0))
                def _():
                    sent(hid.at[slices[f]], zr_s.at[k * shares + f])

                @pl.when((z > 0) & (z + k <= Z - 1))
                def _():
                    sent(hid.at[slices[f]], zl_s.at[k * shares + f])
        sent(hq.at[0:S - 1], pl_s)
        sent(hq, mt_s)
        for b in range(S):
            @pl.when((z >= s) & (z < Z - 1))
            def _():
                sent(cot, cr_s.at[b])

            @pl.when((z <= s) & (z > 0))
            def _():
                sent(cot, cl_s.at[b])

        @pl.when(s != z)
        def _():
            sent(cot, cp_s)
        sent(ids.at[0:S - 1], id_s)
        sent(info.at[0:S - 1], in_s)
        sent(rcv, rs_s)
        sent(cd.at[0:S - 1], ag_s)
        sent(stat_rx.at[0:V - 1], st_s)

    def fin_pass(q, part):
        got(zr.at[q, part], g_r.at[q])
        fin_send(q, zr.at[q, part], part)

    def tied_tile(j, carry):
        rows = pl.ds(pl.multiple_of(j * tile, tile), tile)
        head = emb[rows, :]
        for p in range(S // 2):
            lhs = jnp.concatenate([dl[2 * p, rows, :], dl[2 * p + 1, rows, :]], axis=1)
            head = head + over_tokens(lhs, h[p])
        tied[rows, :] = head.astype(bf16)
        return carry

    begun = tiles // 4
    drain()
    pass_far()

    @pl.when(jnp.logical_not(close))
    def _():
        embed_ready()

    def late_embed(first, last):
        @pl.when(jnp.logical_not(close))
        def _():
            lax.fori_loop(first, last, embed_tile, 0)

    late_embed(0, tiles // 4)
    fin_pass(nx, slice(0, W))
    late_embed(tiles // 4, tiles * 3 // 4)
    fin_pass(ny, slice(0, W))
    late_embed(tiles * 3 // 4, tiles)
    fin_pass(far, lead)
    lax.fori_loop(0, begun, tied_tile, 0)
    gather_far()
    lax.fori_loop(begun, tiles, tied_tile, 0)

    def fin_sum(part):
        for r in range(1, Z):
            u = (z + r) % Z
            got(fin.at[u, part], f_r.at[u])
        acc = fin[0, part].astype(f32)
        for u in range(1, Z):
            acc = acc + fin[u, part].astype(f32)
        hgrad[part] = acc.astype(bf16)

    @pl.when(z == far)
    def _():
        fin_sum(lead)
        got(whole, zw_r)
        hgrad[rest] = whole[...]

    @pl.when(z != far)
    def _():
        fin_sum(slice(0, W))


    for r in range(1, S):
        part = lead if r == 3 else slice(0, W)
        sent(gs.at[0, part], g_s.at[s ^ r])
    for r in range(S):
        part = lead if r == 3 else slice(0, W)

        @pl.when(s ^ r != z)
        def _():
            sent(gs.at[0, part], f_s.at[s ^ r])

    sent(cq, cm_s)
    sent(px_rx, px_s)

    @pl.when(z != s)
    def _():
        sent(gs.at[0, rest], zf_s)

    @pl.when(z == s)
    def _():
        sent(zsum, zw_s)


def put_out(loss, hgrad, tied, loss_out, hgrad_out, tied_out, sems):
    count = sems.shape[0] - 2
    rows = tied.shape[0] // count
    pairs = [(tied.at[pl.ds(n * rows, rows)], tied_out.at[pl.ds(n * rows, rows)]) for n in range(count)]
    pairs += [(hgrad, hgrad_out), (loss, loss_out)]
    moves = [pltpu.make_async_copy(src, dst, sems.at[i]) for i, (src, dst) in enumerate(pairs)]
    for move in moves:
        move.start()
    for move in moves:
        move.wait()


def fused(hidden, slab, token_ids, target_ids, input_cot, loss_grad):
    S = lax.axis_size("section")
    V = lax.axis_size("vocab")
    Z = V // 2
    T, W = hidden.shape
    R, Q = slab.shape
    vm = pltpu.VMEM
    dma = pltpu.SemaphoreType.DMA
    half = vm((S, W, T), bf16)
    both = vm((S // 2, Q, 2 * T), bf16)
    scratch = [
        vm((W, T), bf16), vm((W, T), bf16),
        vm((1, T), jnp.int32), vm((1, T), jnp.int32), vm((1, T), f32),
        vm((R, Q), bf16), half, half, half, both,
        vm((S, R, T), jnp.int16), vm((3, R, T), jnp.int16), vm((R, T), f32),
        half, half, both, vm((S, 8, T), jnp.int32), vm((8, T), jnp.int32),
        vm((S, R, T), jnp.int16), vm((16, T), f32), vm((V, 16, T), f32),
        vm((S, 8, T), f32), vm((S, R, T), bf16), vm((3, T, Q), f32), vm((S, Q, T), f32), vm((S, W, T), f32), half, half, vm((Z, W, T), bf16),
        vm((Z, W // 2, T), bf16), vm((W // 2, T), bf16), vm((W // 2, T), bf16), vm((R, Q), f32),
        dma((6,)), *[dma((Z * shares,))] * 4,
        dma, dma((S * shares,)), dma, dma((S * shares,)), dma, dma((S,)),
        dma((S,)), dma((S,)), dma((S,)), dma, dma, dma, dma,
        dma, dma((S,)),
        dma, dma((3 * steps,)), dma, dma, dma, dma((5 * steps,)),
        dma, dma((S,)), dma((S,)), dma((S,)), dma((Z,)), dma((Z,)),
        dma, dma((Z,)), dma, dma,
    ]
    block = pl.BlockSpec(memory_space=vm)
    anywhere = pl.BlockSpec(memory_space=pl.ANY)
    far_memory = pl.BlockSpec(memory_space=pltpu.HBM)
    results = pl.pallas_call(
        functools.partial(fused_kernel, (S, V)),
        out_shape=(
            jax.ShapeDtypeStruct((1, T), f32),
            jax.ShapeDtypeStruct((W, T), bf16),
            jax.ShapeDtypeStruct((R, Q), bf16),
        ),
        in_specs=[far_memory] * 6,
        out_specs=(block, block, block),
        scratch_shapes=scratch,
        compiler_params=pltpu.CompilerParams(
            collective_id=0, has_side_effects=True, vmem_limit_bytes=48 * 2**20
        ),
        name="fused",
    )(
        *(
            pltpu.with_memory_space_constraint(x, pltpu.HBM)
            for x in (
                hidden.T, input_cot.T, slab,
                token_ids.reshape(1, T), target_ids.reshape(1, T), loss_grad.reshape(1, T),
            )
        )
    )
    loss, hgrad, tied = pl.pallas_call(
        put_out,
        out_shape=tuple(jax.ShapeDtypeStruct(x.shape, x.dtype) for x in results),
        in_specs=[block] * 3,
        out_specs=(anywhere,) * 3,
        scratch_shapes=[dma((10,))],
        compiler_params=pltpu.CompilerParams(vmem_limit_bytes=8 * 2**20),
        name="put_out",
    )(*results)
    return loss.reshape(T), hgrad.T, tied


def from_partner(block, axis, stride):
    count = lax.axis_size(axis)
    route = []
    for low in range(count):
        high = low | 1 << stride
        if high != low and high < count:
            route += [(low, high), (high, low)]
    return lax.ppermute(block, axis, route)


def left_product(left_side, right_side):
    return lax.dot_general(
        left_side, right_side, (((0,), (0,)), ((), ())), preferred_element_type=jnp.float32
    )


def local_parts(raw_logits, targets, columns):
    capped = logit_cap * jnp.tanh(raw_logits / logit_cap)
    exp_logits = jnp.exp(capped)
    target_hit = (targets[:, None] == columns[None, :]).astype(jnp.float32)
    local_total = jnp.sum(exp_logits, axis=1)
    local_pick = jnp.sum(target_hit * capped, axis=1)
    return (capped, exp_logits, target_hit, local_total, local_pick)


def finish(capped, exp_logits, target_hit, exp_total, picked, scales):
    token_loss = jnp.log(exp_total) - picked
    slope = 1.0 - (capped / logit_cap) ** 2
    dlogit = (scales[:, None] * (exp_logits / exp_total[:, None] - target_hit) * slope).astype(
        jnp.bfloat16
    )
    return (token_loss, dlogit)


def general(hidden, slab, token_ids, target_ids, input_cot, loss_grad):
    rows_here = slab.shape[0]
    quarter_width = slab.shape[1]
    sections = lax.axis_size("section")
    shards = lax.axis_size("vocab")
    model_width = quarter_width * sections
    own_tokens = hidden.shape[0]
    share_width = hidden.shape[1]
    full_hidden, full_cot = (
        lax.all_gather(hidden, "vocab", axis=1, tiled=True),
        lax.all_gather(input_cot, "vocab", axis=1, tiled=True),
    )
    hidden_part, cot_part = (
        lax.all_to_all(full_hidden, "section", split_axis=1, concat_axis=0, tiled=True),
        lax.all_to_all(full_cot, "section", split_axis=1, concat_axis=0, tiled=True),
    )
    partial_value = lax.dot_general(
        hidden_part, slab, (((1,), (1,)), ((), ())), preferred_element_type=jnp.float32
    )
    columns = lax.axis_index("vocab") * rows_here + jnp.arange(rows_here, dtype=jnp.int32)
    raw_logits = lax.psum_scatter(partial_value, "section", scatter_dimension=0, tiled=True)
    capped, exp_logits, target_hit, local_total, local_pick = local_parts(
        raw_logits, target_ids, columns
    )
    exp_total, picked = lax.psum((local_total, local_pick), "vocab")
    token_loss, dlogit = finish(capped, exp_logits, target_hit, exp_total, picked, loss_grad)
    all_ids = lax.all_gather(token_ids, "section", axis=0, tiled=True)
    all_dlogit = lax.all_gather(dlogit, "section", axis=0, tiled=True)
    total_tokens = all_dlogit.shape[0]
    blocks = shards // sections
    narrow = share_width // sections
    arranged_slab = slab.reshape(rows_here, blocks, sections, narrow)
    term = jnp.einsum(
        "tv,vkrw->trkw", all_dlogit, arranged_slab, preferred_element_type=jnp.float32
    )
    term = term.reshape(total_tokens, shards * narrow)
    piece = lax.psum_scatter(term, "vocab", scatter_dimension=1, tiled=True).astype(jnp.bfloat16)
    slots = lax.all_to_all(piece, "section", split_axis=0, concat_axis=0, tiled=True).reshape(
        sections, own_tokens, narrow
    )
    base_bit = blocks.bit_length() - 1
    rank_high = lax.axis_index("vocab") // blocks
    for level in range(sections.bit_length() - 1):
        span = 1 << level
        shaped = slots.reshape(sections // (2 * span), 2, span, own_tokens, narrow)
        mine_bit = rank_high // span % 2
        lower = shaped[:, 0]
        upper = shaped[:, 1]
        keep = jnp.where(mine_bit == 0, lower, upper)
        outgoing = jnp.where(mine_bit == 0, upper, lower)
        incoming = from_partner(outgoing, "vocab", base_bit + level)
        first = jnp.where(mine_bit == 0, keep, incoming)
        second = jnp.where(mine_bit == 0, incoming, keep)
        slots = jnp.stack([first, second], axis=1).reshape(sections, own_tokens, narrow)
    hidden_grad = jnp.transpose(slots, (1, 0, 2)).reshape(own_tokens, sections * narrow)
    onehot = (all_ids[:, None] == columns[None, :]).astype(jnp.bfloat16)
    embed_scale = math.sqrt(model_width)
    tied_grad = left_product(all_dlogit, hidden_part) + left_product(onehot, cot_part) * embed_scale
    return (token_loss, hidden_grad, tied_grad.astype(jnp.bfloat16))


def on_device(hidden, slab, token_ids, target_ids, input_cot, loss_grad):
    sections = lax.axis_size("section")
    shards = lax.axis_size("vocab")
    fits = (
        sections == 4
        and shards == 2 * sections
        and hidden.shape[0] % 128 == 0
        and slab.shape[0] % 2048 == 0
        and hidden.shape[1] % 32 == 0
    )
    step = fused if fits else general
    return step(hidden, slab, token_ids, target_ids, input_cot, loss_grad)


def solution(mesh):
    placed = (
        P("section", "vocab"),
        P("vocab", "section"),
        P("section"),
        P("section"),
        P("section", "vocab"),
        P("section"),
    )
    return jax.shard_map(
        on_device,
        mesh=mesh,
        in_specs=placed,
        out_specs=(P("section"), P("section", "vocab"), P("vocab", "section")),
        check_vma=False,
    )
```
